32 devices in a mesh: part: 2 (over x), row: 4 (over z), col: 4 (over y, core).
Axes of the slice: x: 2, y: 2, z: 4, core: 2. Of those that a mesh axis runs over, the one named last changes fastest.
Arguments:
- ratings: float32 [1024, 32768], P(('part', 'row'), 'col'), parts along dimension 0
- mask: int32 [1024, 32768], P(('part', 'row'), 'col'), parts along dimension 0
- user_init: float32 [1024, 64], P(('part', 'row')), parts along dimension 0
- item_init: float32 [65536, 64], P(('part', 'col')), parts along dimension 0
Outputs:
- output 1: float32 [1024, 64], P(('part', 'row')), parts along dimension 0
- output 2: float32 [65536, 64], P(('part', 'col')), parts along dimension 0
There are 2 independent parts. The reference program is written for one: setup_inputs(seed, part) draws one part's arguments, and reference() takes and returns one part's arrays. A program takes and returns all parts, laid end to end along the dimension named above; each array names one.
All inputs are finite; a program needn't handle non-finite values.
Results may differ from the reference program's by a relative error of at most 0.00388836.
Values are sent between devices in bfloat16 or wider.
A program may use at most 1 GiB of HBM per device.

```python
import jax
import jax.numpy as jnp

RANK_DIM = 64
NUM_USERS = 512
NUM_ITEMS = 32768
CG_STEPS = 4
RIDGE_WEIGHT = 0.0005


def setup_inputs(seed: int = 0, part: int = 0) -> dict:
    root_key = jax.random.fold_in(jax.random.key(seed), part)
    sub_keys = jax.random.split(root_key, 7)
    user_true = jax.random.normal(sub_keys[0], (NUM_USERS, RANK_DIM), jnp.float32)
    item_true = jax.random.normal(sub_keys[1], (NUM_ITEMS, RANK_DIM), jnp.float32)
    rating_noise = jax.random.normal(sub_keys[2], (NUM_USERS, NUM_ITEMS), jnp.float32)
    ratings = jnp.dot(user_true, item_true.T) * RANK_DIM ** -0.5 + 0.5 * rating_noise
    density = jax.random.randint(sub_keys[3], (NUM_USERS, 1), 30, 71)
    mask = (jax.random.randint(sub_keys[4], (NUM_USERS, NUM_ITEMS), 0, 100) < density).astype(jnp.int32)
    col_scale = 8.0 ** (-jnp.arange(RANK_DIM, dtype=jnp.float32) / (RANK_DIM - 1))
    item_noise = jax.random.normal(sub_keys[5], (NUM_ITEMS, RANK_DIM), jnp.float32)
    item_init = (item_true + 0.5 * item_noise) * col_scale * RANK_DIM ** -0.25
    user_init = 2.0 * jax.random.normal(sub_keys[6], (NUM_USERS, RANK_DIM), jnp.float32) * RANK_DIM ** -0.25
    return {"ratings": ratings, "mask": mask, "user_init": user_init, "item_init": item_init}


def cg_solve(mask_on, ratings, fixed_fac, start, ridge):
    fixed_bf = fixed_fac.astype(jnp.bfloat16)
    mask_bf = mask_on.astype(jnp.bfloat16)
    scores = jnp.dot(start.astype(jnp.bfloat16), fixed_bf.T, preferred_element_type=jnp.float32)
    resid_obs = jnp.where(mask_on, ratings - scores, 0.0).astype(jnp.bfloat16)
    residual = jnp.dot(resid_obs, fixed_bf, preferred_element_type=jnp.float32) - ridge * start
    direction = residual
    estimate = start
    res_sq = jnp.sum(residual * residual, axis=1, keepdims=True)
    for cg_step in range(CG_STEPS):
        scores = jnp.dot(direction.astype(jnp.bfloat16), fixed_bf.T, preferred_element_type=jnp.float32)
        masked = mask_bf * scores.astype(jnp.bfloat16)
        gram_dir = jnp.dot(masked, fixed_bf, preferred_element_type=jnp.float32) + ridge * direction
        step_size = res_sq / jnp.sum(direction * gram_dir, axis=1, keepdims=True)
        estimate = estimate + step_size * direction
        if cg_step + 1 < CG_STEPS:
            residual = residual - step_size * gram_dir
            new_sq = jnp.sum(residual * residual, axis=1, keepdims=True)
            direction = residual + (new_sq / res_sq) * direction
            res_sq = new_sq
    return estimate


def reference(ratings, mask, user_init, item_init):
    mask_on = mask > 0
    user_new = cg_solve(mask_on, ratings, item_init, user_init, RIDGE_WEIGHT * NUM_ITEMS)
    item_new = cg_solve(mask_on.T, ratings.T, user_new, item_init, RIDGE_WEIGHT * NUM_USERS)
    return (user_new, item_new)
```

```python
import jax
import jax.numpy as jnp
from jax import lax
from jax.sharding import PartitionSpec as P

CG_STEPS = 4
RIDGE_WEIGHT = 0.0005
BF, F32 = jnp.bfloat16, jnp.float32


def mm(a, b, dims):
    return lax.dot_general(a, b, (dims, ((), ())), preferred_element_type=F32)


def cg_steps(apply_a, start, residual, axis):
    direction = residual
    estimate = start
    res_sq = jnp.sum(residual * residual, axis=axis, keepdims=True)
    for cg_step in range(CG_STEPS):
        gram_dir = apply_a(direction)
        step_size = res_sq / jnp.sum(direction * gram_dir, axis=axis, keepdims=True)
        estimate = estimate + step_size * direction
        if cg_step + 1 < CG_STEPS:
            residual = residual - step_size * gram_dir
            new_sq = jnp.sum(residual * residual, axis=axis, keepdims=True)
            direction = residual + (new_sq / res_sq) * direction
            res_sq = new_sq
    return estimate


def solution(mesh):
    row_size = mesh.shape["row"]
    col_size = mesh.shape["col"]
    grid_spec = P(("part", "row"), "col")
    user_spec = P(("part", "row"), None)
    item_spec = P(("part", "col"), None)

    def local_step(ratings, mask, user_blk, item_blk):
        users_part = ratings.shape[0] * row_size
        items_part = ratings.shape[1] * col_size
        items_own = ratings.shape[1] // row_size
        mask_on = mask > 0
        mask_bf = mask_on.astype(BF)
        mask_item = lax.all_to_all(mask_bf, "row", split_axis=1, concat_axis=0, tiled=True)
        user_t, item_t = user_blk.T, item_blk.T

        item_bf = item_t.astype(BF)
        ridge = RIDGE_WEIGHT * items_part
        scores = mm(user_t.astype(BF), item_bf, ((0,), (0,)))
        obs = jnp.where(mask_on, ratings - scores, 0.0).astype(BF)
        residual = lax.psum(mm(item_bf, obs, ((1,), (1,))), "col") - ridge * user_t

        def apply_user(x):
            scores = mm(x.astype(BF), item_bf, ((0,), (0,)))
            masked = mask_bf * scores.astype(BF)
            return lax.psum(mm(item_bf, masked, ((1,), (1,))), "col") + ridge * x

        user_new = cg_steps(apply_user, user_t, residual, 0)

        ridge_i = RIDGE_WEIGHT * users_part
        own_bf = user_new.astype(BF)
        all_bf = lax.all_gather(own_bf, "row", axis=1, tiled=True)
        scores = mm(own_bf, item_bf, ((0,), (0,)))
        obs = jnp.where(mask_on, ratings - scores, 0.0).astype(BF)
        part = mm(own_bf, obs, ((1,), (0,)))
        start = lax.dynamic_slice_in_dim(item_t, lax.axis_index("row") * items_own, items_own, 1)
        residual = lax.psum_scatter(part, "row", scatter_dimension=1, tiled=True) - ridge_i * start

        def apply_item(x):
            scores = mm(all_bf, x.astype(BF), ((0,), (0,)))
            masked = mask_item * scores.astype(BF)
            return mm(all_bf, masked, ((1,), (0,))) + ridge_i * x

        item_new = cg_steps(apply_item, start, residual, 0)
        item_new = lax.all_gather(item_new, "row", axis=1, tiled=True)
        return user_new.T, item_new.T

    return jax.shard_map(local_step, mesh=mesh, in_specs=(grid_spec, grid_spec, user_spec, item_spec), out_specs=(user_spec, item_spec), check_vma=False)
```

```python
import functools

import jax
import jax.numpy as jnp
from jax import lax
from jax.experimental import pallas as pl
from jax.experimental.pallas import tpu as pltpu
from jax.sharding import PartitionSpec as P

CG_STEPS = 4
RIDGE_WEIGHT = 0.0005
CHUNKS = 4
BF, F32 = jnp.bfloat16, jnp.float32
MESH = pl.DeviceIdType.MESH


def mm(a, b, contract_a, contract_b):
    return lax.dot_general(a, b, (((contract_a,), (contract_b,)), ((), ())), preferred_element_type=F32)


def col_sum(a, b):
    return jnp.sum(a * b, axis=0, keepdims=True)


def cg_steps(apply_a, start, residual):
    direction = residual
    estimate = start
    res_sq = col_sum(residual, residual)
    for cg_step in range(CG_STEPS):
        gram_dir = apply_a(cg_step, direction)
        step_size = res_sq / col_sum(direction, gram_dir)
        estimate = estimate + step_size * direction
        if cg_step + 1 < CG_STEPS:
            residual = residual - step_size * gram_dir
            new_sq = col_sum(residual, residual)
            direction = residual + (new_sq / res_sq) * direction
            res_sq = new_sq
    return estimate


def kernel(
    ridge_u, ridge_i,
    r_hbm, m_hbm, w0_ref, v0_hbm,
    u_out, v_out,
    mint, rbuf, v0b, fb, mown, mrecv, ar, wg, wrow, part, rec_e, rec_x, vout,
    ld_sem, ms_sem, mr_sem, as_sem, arr_sem, ws_sem, wr_sem, rs_sem, re_sem, rx_sem, ag_sem, agr_sem, out_sem,
):
    z = lax.axis_index("row")
    c = lax.axis_index("col")
    blk = mint.shape[2]
    nc, width = part.shape[1], part.shape[3]
    hi = z // 2
    is_mid = lax.rem(z + hi, 2)

    def row_of(mirrored):
        return mirrored + hi * (3 - 2 * mirrored)

    def to_row(src, dst, send, recv, row):
        return pltpu.make_async_remote_copy(
            src_ref=src, dst_ref=dst, send_sem=send, recv_sem=recv, device_id={"row": row}, device_id_type=MESH)

    order = (1 + lax.rem(z, 2), lax.rem(z + 2, 4), 3 - 3 * lax.rem(z, 2), z)

    def load(hbm, buf, kind, s):
        return pltpu.make_async_copy(
            hbm.at[:, pl.ds(pl.multiple_of(s * blk, blk), blk)], buf.at[s], ld_sem.at[kind, s])

    for s in order:
        load(m_hbm, mint, 0, s).start()
    for s in range(4):
        load(v0_hbm, v0b, 1, s).start()
    for s in range(4):
        load(r_hbm, rbuf, 2, s).start()

    barrier = pltpu.get_barrier_semaphore()
    for off in range(1, 4):
        pl.semaphore_signal(barrier, inc=1, device_id={"row": lax.rem(z + off, 4)}, device_id_type=MESH)
        pl.semaphore_signal(barrier, inc=1, device_id={"col": lax.rem(c + off, 4)}, device_id_type=MESH)
    pl.semaphore_wait(barrier, 6)

    for j, s in enumerate(order):
        load(m_hbm, mint, 0, s).wait()
        for k in range(nc):
            m = mint[s, :, k * width:(k + 1) * width].astype(F32).astype(BF)
            mown[s, k] = m
            if j == 3:
                mrecv[z, k] = m
        if j < 3:
            to_row(mown.at[s], mrecv.at[z], ms_sem.at[s], mr_sem.at[z], s).start()

    for s in range(4):
        load(v0_hbm, v0b, 1, s).wait()
        fb[s] = v0b[s].astype(BF)
    for s in range(4):
        load(r_hbm, rbuf, 2, s).wait()

    def observed(s, k, scores):
        cols = slice(k * width, (k + 1) * width)
        return jnp.where(mint[s, :, cols] > 0, rbuf[s, :, cols] - scores, 0.0).astype(BF)

    def user_product(x, residual):
        rows = x.T.astype(BF)

        def block(s, acc):
            for k in range(nc):
                f = fb[s, :, k * width:(k + 1) * width]
                scores = mm(rows, f, 1, 0)
                masked = observed(s, k, scores) if residual else mown[s, k] * scores.astype(BF)
                acc = acc + mm(f, masked, 1, 1)
            return acc

        return lax.fori_loop(0, 4, block, jnp.zeros(x.shape, F32))

    def to_col(rnd, off):
        peer = lax.rem(c + off, 4)
        return pltpu.make_async_remote_copy(
            src_ref=ar.at[rnd, c], dst_ref=ar.at[rnd, c], send_sem=as_sem.at[rnd, off], recv_sem=arr_sem.at[rnd, c],
            device_id={"col": peer}, device_id_type=MESH)

    def from_col(rnd, off):
        peer = lax.rem(c + off, 4)
        return pltpu.make_async_remote_copy(
            src_ref=ar.at[rnd, peer], dst_ref=ar.at[rnd, peer], send_sem=as_sem.at[rnd, off],
            recv_sem=arr_sem.at[rnd, peer], device_id={"col": peer}, device_id_type=MESH)

    def sum_cols(rnd, x):
        ar[rnd, c] = x
        for off in range(1, 4):
            to_col(rnd, off).start()
        for off in range(1, 4):
            from_col(rnd, off).wait_recv()
        return (ar[rnd, 0] + ar[rnd, 1]) + (ar[rnd, 2] + ar[rnd, 3])

    w0 = w0_ref[...]
    res = sum_cols(0, user_product(w0, True)) - ridge_u * w0
    w1 = cg_steps(lambda i, p: sum_cols(i + 1, user_product(p, False)) + ridge_u * p, w0, res)
    u_out[...] = w1

    wg[z] = w1.astype(BF)
    for off in range(1, 4):
        peer = lax.rem(z + off, 4)
        to_row(wg.at[z], wg.at[z], ws_sem.at[peer], wr_sem.at[z], peer).start()

    own_rows = w1.T.astype(BF)
    own_cols = w1.astype(BF)

    def rs_out(s, k):
        return to_row(part.at[s, k], rec_e.at[s, k], rs_sem.at[s, k], re_sem.at[s, k], 1 + hi)

    def rs_cross(s, k):
        return to_row(part.at[s, k], rec_x.at[s, k], rs_sem.at[s, k], rx_sem.at[s, k], 3 - z)

    def rs_end(s, k):
        return to_row(part.at[s, k], rec_x.at[s, k], rs_sem.at[s, k], rx_sem.at[s, k], 3 * hi)

    def partial_sums(j, carry):
        mirrored = 3 - j + is_mid * (j // 2) * (2 * j - 5)
        s = row_of(mirrored)
        for k in range(nc):
            scores = mm(own_rows, fb[s, :, k * width:(k + 1) * width], 1, 0)
            part[s, k] = mm(own_cols, observed(s, k, scores), 1, 0)

        @pl.when((is_mid == 0) & (j < 3))
        def _():
            for k in range(nc):
                rs_out(s, k).start()

        return carry

    lax.fori_loop(0, 4, partial_sums, 0)

    for off in range(1, 4):
        peer = lax.rem(z + off, 4)
        to_row(wg.at[peer], wg.at[peer], ws_sem.at[peer], wr_sem.at[peer], peer).wait_recv()
        to_row(mown.at[peer], mrecv.at[peer], ms_sem.at[peer], mr_sem.at[peer], peer).wait_recv()
    for s in range(4):
        wrow[s] = wg[s].astype(F32).T.astype(BF)

    def solve_items(k, residual):
        start = v0b[z, :, pl.ds(pl.multiple_of(k * width, width), width)]

        def apply_a(i, p):
            pb = p.astype(BF)
            acc = ridge_i * p
            for s in range(0, 4, 2):
                scores = [mrecv[t, k] * mm(wrow[t], pb, 1, 0).astype(BF) for t in (s, s + 1)]
                both = jnp.concatenate([wg[s], wg[s + 1]], axis=1)
                acc = acc + mm(both, jnp.concatenate(scores, axis=0), 1, 0)
            return acc

        vout[z, k] = cg_steps(apply_a, start, residual - ridge_i * start)

    def ag(s, k, row, lane):
        return to_row(vout.at[s, k], vout.at[s, k], ag_sem.at[lane, s, k], agr_sem.at[s, k], row)

    def save(s, k):
        cols = pl.ds(pl.multiple_of(s * blk + k * width, width), width)
        return pltpu.make_async_copy(vout.at[s, k], v_out.at[:, cols], out_sem.at[s, k])

    def each(body):
        def step(k, carry):
            body(k)
            return carry

        lax.fori_loop(0, nc, step, 0)

    s0, s1, s2, s3 = (row_of(m) for m in range(4))

    @pl.when(is_mid == 0)
    def _():
        inner = 1 + hi

        def own(k):
            rs_end(s0, k).wait_recv()
            solve_items(k, part[s0, k] + rec_x[s0, k])
            ag(s0, k, inner, 0).start()
            save(s0, k).start()

        def take(s):
            def body(k):
                ag(s, k, inner, 0).wait_recv()
                save(s, k).start()

            return body

        def drain(k):
            for s in (s1, s2, s3):
                rs_out(s, k).wait_send()
            ag(s0, k, inner, 0).wait_send()

        each(own)
        for s in (s1, s2, s3):
            each(take(s))
        each(drain)

    @pl.when(is_mid == 1)
    def _():
        end, cross = 3 * hi, 3 - z

        def outer_to_cross(s):
            def body(k):
                rs_out(s, k).wait_recv()
                part[s, k] = part[s, k] + rec_e[s, k]
                rs_cross(s, k).start()

            return body

        def cross_to_end(k):
            rs_cross(s0, k).wait_recv()
            part[s0, k] = part[s0, k] + rec_x[s0, k]
            rs_end(s0, k).start()

        def own(k):
            rs_out(s1, k).wait_recv()
            rs_cross(s1, k).wait_recv()
            solve_items(k, part[s1, k] + (rec_e[s1, k] + rec_x[s1, k]))
            ag(s1, k, cross, 0).start()
            ag(s1, k, end, 1).start()
            save(s1, k).start()

        def relay(s, row):
            def body(k):
                ag(s, k, row, 0).wait_recv()
                ag(s, k, row, 0).start()
                save(s, k).start()

            return body

        def drain(k):
            for s in (s3, s2):
                rs_cross(s, k).wait_send()
            rs_end(s0, k).wait_send()
            ag(s1, k, cross, 0).wait_send()
            ag(s1, k, end, 1).wait_send()
            ag(s0, k, cross, 0).wait_send()
            ag(s2, k, end, 0).wait_send()
            ag(s3, k, end, 0).wait_send()

        each(outer_to_cross(s3))

        def both(k):
            outer_to_cross(s2)(k)
            cross_to_end(k)

        each(both)
        each(own)

        def relays(k):
            relay(s0, cross)(k)
            relay(s2, end)(k)

        each(relays)
        each(relay(s3, end))
        each(drain)

    for off in range(1, 4):
        peer = lax.rem(z + off, 4)
        to_row(wg.at[z], wg.at[z], ws_sem.at[peer], wr_sem.at[z], peer).wait_send()
        to_row(mown.at[peer], mrecv.at[z], ms_sem.at[peer], mr_sem.at[z], peer).wait_send()
        for rnd in range(CG_STEPS + 1):
            to_col(rnd, off).wait_send()
    for s in range(4):
        each(lambda k: save(s, k).wait())


def solution(mesh):
    row_size = mesh.shape["row"]
    col_size = mesh.shape["col"]
    assert row_size == 4 and col_size == 4
    grid_spec = P(("part", "row"), "col")
    user_spec = P(("part", "row"), None)
    item_spec = P(("part", "col"), None)

    def local_step(ratings, mask, user_blk, item_blk):
        users, items = ratings.shape
        rank = user_blk.shape[1]
        blk = items // row_size
        width = blk // CHUNKS
        ridge_u, ridge_i = RIDGE_WEIGHT * (items * col_size), RIDGE_WEIGHT * (users * row_size)
        vmem, any_space = pl.BlockSpec(memory_space=pltpu.VMEM), pl.BlockSpec(memory_space=pl.ANY)
        dma = pltpu.SemaphoreType.DMA
        sums = pltpu.VMEM((4, CHUNKS, rank, width), F32)
        user_new, item_new = pl.pallas_call(
            functools.partial(kernel, ridge_u, ridge_i),
            out_shape=(jax.ShapeDtypeStruct((rank, users), F32), jax.ShapeDtypeStruct((rank, items), F32)),
            in_specs=[any_space, any_space, vmem, any_space],
            out_specs=(vmem, any_space),
            scratch_shapes=[
                pltpu.VMEM((4, users, blk), jnp.int32),
                pltpu.VMEM((4, users, blk), F32),
                pltpu.VMEM((4, rank, blk), F32),
                pltpu.VMEM((4, rank, blk), BF),
                pltpu.VMEM((4, CHUNKS, users, width), BF),
                pltpu.VMEM((4, CHUNKS, users, width), BF),
                pltpu.VMEM((CG_STEPS + 1, 4, rank, users), F32),
                pltpu.VMEM((4, rank, users), BF),
                pltpu.VMEM((4, users, rank), BF),
                sums, sums, sums, sums,
                dma((3, 4)), dma((4,)), dma((4,)), dma((CG_STEPS + 1, 4)), dma((CG_STEPS + 1, 4)), dma((4,)), dma((4,)),
                dma((4, CHUNKS)), dma((4, CHUNKS)), dma((4, CHUNKS)), dma((2, 4, CHUNKS)), dma((4, CHUNKS)), dma((4, CHUNKS)),
            ],
            compiler_params=pltpu.CompilerParams(
                collective_id=0, has_side_effects=True, vmem_limit_bytes=56 * 2**20),
            name="als_sweep",
        )(ratings, mask, user_blk.T, item_blk.T)
        return user_new.T, item_new.T

    return jax.shard_map(local_step, mesh=mesh, in_specs=(grid_spec, grid_spec, user_spec, item_spec), out_specs=(user_spec, item_spec), check_vma=False)
```

```python
import functools

import jax
import jax.numpy as jnp
from jax import lax
from jax.experimental import pallas as pl
from jax.experimental.pallas import tpu as pltpu
from jax.sharding import PartitionSpec as P

CG_STEPS = 4
RIDGE_WEIGHT = 0.0005
CHUNKS = 8
CROSS_STEP = 1
OUT_AT, END_AT, OWN_AT, NEAR_AT, OUTER_AT, FAR_AT = (0, 3), (8, 2), (9, 2), (13, 2), (23, 1), (26, 1)
BF, F32 = jnp.bfloat16, jnp.float32
MESH = pl.DeviceIdType.MESH


def mm(a, b, contract_a, contract_b):
    return lax.dot_general(a, b, (((contract_a,), (contract_b,)), ((), ())), preferred_element_type=F32)


def col_sum(a, b):
    return jnp.sum(a * b, axis=0, keepdims=True)


def cg_steps(apply_a, start, residual):
    direction = residual
    estimate = start
    res_sq = col_sum(residual, residual)
    for cg_step in range(CG_STEPS):
        gram_dir = apply_a(direction)
        step_size = res_sq / col_sum(direction, gram_dir)
        estimate = estimate + step_size * direction
        if cg_step + 1 < CG_STEPS:
            residual = residual - step_size * gram_dir
            new_sq = col_sum(residual, residual)
            direction = residual + (new_sq / res_sq) * direction
            res_sq = new_sq
    return estimate


def kernel(
    ridge_u, ridge_i,
    r_hbm, m_hbm, w0_ref, v0_hbm,
    u_out, vout,
    mint, rbuf, v0b, fb, mown, mrecv, ar, wg, wrow, wcol, part, rec_e, rec_x,
    ld_sem, ms_sem, mr_sem, as_sem, arr_sem, ws_sem, wr_sem, rs_sem, re_sem, rx_sem, ag_sem, agr_sem,
):
    z = lax.axis_index("row")
    c = lax.axis_index("col")
    blk = mint.shape[2]
    nc, width = part.shape[1], part.shape[3]
    hi = z // 2
    is_mid = lax.rem(z + hi, 2)

    def row_of(mirrored):
        return mirrored + hi * (3 - 2 * mirrored)

    def to_row(src, dst, send, recv, row):
        return pltpu.make_async_remote_copy(
            src_ref=src, dst_ref=dst, send_sem=send, recv_sem=recv, device_id={"row": row}, device_id_type=MESH)

    def sent(buf, sem, n):
        src = buf if n is None or n == 1 else buf.at[:n]
        to_row(src, src, sem, sem, z).wait_send()

    cross, end = 3 - z, 3 * hi
    order = (3 - z, lax.rem(z + 2, 4), is_mid * end + (1 - is_mid) * (1 + hi), z)

    def load(hbm, buf, kind, s):
        return pltpu.make_async_copy(
            hbm.at[:, pl.ds(pl.multiple_of(s * blk, blk), blk)], buf.at[s], ld_sem.at[kind, s])

    barrier = pltpu.get_barrier_semaphore()
    load(m_hbm, mint, 0, order[0]).start()
    for off in (2, 3, 1):
        pl.semaphore_signal(barrier, inc=1, device_id={"row": lax.rem(z + off, 4)}, device_id_type=MESH)
    for off in range(1, 4):
        pl.semaphore_signal(barrier, inc=1, device_id={"col": lax.rem(c + off, 4)}, device_id_type=MESH)
    load(v0_hbm, v0b, 1, order[0]).start()
    load(r_hbm, rbuf, 2, order[0]).start()
    for s in order[1:]:
        load(m_hbm, mint, 0, s).start()
        load(v0_hbm, v0b, 1, s).start()
        load(r_hbm, rbuf, 2, s).start()

    def observed(s, k, scores):
        cols = pl.ds(pl.multiple_of(k * width, width), width)
        return jnp.where(mint[s, :, cols] > 0, rbuf[s, :, cols] - scores, 0.0).astype(BF)

    def send_mask(s):
        to_row(mown.at[s], mrecv.at[z], ms_sem, mr_sem.at[z], s).start()

    w0 = w0_ref[...]
    rows0 = w0.T.astype(BF)
    first = jnp.zeros((w0.shape[1], w0.shape[0]), F32)
    for j, s in enumerate(order):
        load(m_hbm, mint, 0, s).wait()
        for k in range(nc):
            m = mint[s, :, k * width:(k + 1) * width].astype(F32).astype(BF)
            mown[s, k] = m
            if j == 3:
                mrecv[z, k] = m
        if j == 0:
            pl.semaphore_wait(barrier, 6)
        if j == 2:
            send_mask(s)
        elif j < 2:
            @pl.when(is_mid == 0)
            def _():
                send_mask(s)
        load(v0_hbm, v0b, 1, s).wait()
        load(r_hbm, rbuf, 2, s).wait()
        for k in range(nc):
            cols = slice(k * width, (k + 1) * width)
            f = v0b[s, :, cols].astype(BF)
            fb[s, :, cols] = f
            first = first + mm(observed(s, k, mm(rows0, f, 1, 0)), f, 1, 1)

    def user_product(x):
        rows = x.T.astype(BF)
        acc = jnp.zeros((x.shape[1], x.shape[0]), F32)
        for s in range(4):
            for k in range(0, nc, 2):
                f = fb[s, :, k * width:(k + 2) * width]
                mask = jnp.concatenate([mown[s, k], mown[s, k + 1]], axis=1)
                acc = acc + mm(mask * mm(rows, f, 1, 0).astype(BF), f, 1, 1)
        return acc.T

    def to_col(rnd, off):
        peer = lax.rem(c + off, 4)
        return pltpu.make_async_remote_copy(
            src_ref=ar.at[rnd, c], dst_ref=ar.at[rnd, c], send_sem=as_sem, recv_sem=arr_sem.at[rnd, c],
            device_id={"col": peer}, device_id_type=MESH)

    def from_col(rnd, off):
        peer = lax.rem(c + off, 4)
        return pltpu.make_async_remote_copy(
            src_ref=ar.at[rnd, peer], dst_ref=ar.at[rnd, peer], send_sem=as_sem,
            recv_sem=arr_sem.at[rnd, peer], device_id={"col": peer}, device_id_type=MESH)

    def sum_cols(rnd, x):
        ar[rnd, c] = x
        for off in range(1, 4):
            to_col(rnd, off).start()
        for off in range(1, 4):
            from_col(rnd, off).wait_recv()
        return (ar[rnd, 0] + ar[rnd, 1]) + (ar[rnd, 2] + ar[rnd, 3])

    res = sum_cols(0, first.T) - ridge_u * w0

    def user_step(i, state):
        x, r, p, res_sq = state

        @pl.when((is_mid == 1) & (i == CROSS_STEP))
        def _():
            for s in order[:2]:
                send_mask(s)

        q = sum_cols(i + 1, user_product(p)) + ridge_u * p
        step_size = res_sq / col_sum(p, q)
        x = x + step_size * p
        r = r - step_size * q
        new_sq = col_sum(r, r)
        p = r + (new_sq / res_sq) * p
        return x, r, p, new_sq

    w1 = lax.fori_loop(0, CG_STEPS, user_step, (w0, res, res, col_sum(res, res)))[0]
    u_out[...] = w1

    wg[z] = w1.astype(BF)
    for off in range(1, 4):
        peer = lax.rem(z + off, 4)
        to_row(wg.at[z], wg.at[z], ws_sem, wr_sem.at[z], peer).start()

    own_rows = w1.T.astype(BF)
    own_cols = w1.astype(BF)

    def rs_out(s, k):
        return to_row(part.at[s, k], rec_e.at[s, k], rs_sem, re_sem.at[s, k], 1 + hi)

    def rs_cross(s, k):
        return to_row(part.at[s, k], rec_x.at[s, k], rs_sem, rx_sem.at[s, k], 3 - z)

    def rs_end(s, k):
        return to_row(part.at[s, k], rec_x.at[s, k], rs_sem, rx_sem.at[s, k], 3 * hi)

    def each(body, n=nc):
        def step(k, carry):
            body(k)
            return carry

        lax.fori_loop(0, n, step, 0)

    def outer_first(j):
        return row_of(3 - j)

    def partial_sums(k):
        for j in range(4):
            s = outer_first(j)
            f = fb[s, :, pl.ds(pl.multiple_of(k * width, width), width)]
            part[s, k] = mm(own_cols, observed(s, k, mm(own_rows, f, 1, 0)), 1, 0)

        @pl.when(is_mid == 0)
        def _():
            for j in range(3):
                rs_out(outer_first(j), k).start()

    each(partial_sums)

    def gather():
        for off in range(1, 4):
            peer = lax.rem(z + off, 4)
            to_row(wg.at[peer], wg.at[peer], ws_sem, wr_sem.at[peer], peer).wait_recv()
            to_row(mown.at[peer], mrecv.at[peer], ms_sem, mr_sem.at[peer], peer).wait_recv()
        users = own_rows.shape[0]
        for s in range(4):
            wrow[s * users:(s + 1) * users] = wg[s].astype(F32).T.astype(BF)
            wcol[:, s * users:(s + 1) * users] = wg[s]

    def cols_of(s, k):
        return pl.ds(pl.multiple_of(s * blk + k * width, width), width)

    def solve_items(k, residual):
        start = v0b[z, :, pl.ds(pl.multiple_of(k * width, width), width)]

        def apply_a(p):
            masked = jnp.concatenate([mrecv[t, k] for t in range(4)], axis=0)
            masked = masked * mm(wrow[...], p.astype(BF), 1, 0).astype(BF)
            return mm(wcol[...], masked, 1, 0) + ridge_i * p

        vout[:, cols_of(z, k)] = cg_steps(apply_a, start, residual - ridge_i * start)

    def ag(s, k, row):
        chunk = vout.at[:, cols_of(s, k)]
        return to_row(chunk, chunk, ag_sem, agr_sem.at[s, k], row)

    s0, s1, s2, s3 = (row_of(m) for m in range(4))

    @pl.when(is_mid == 0)
    def _():
        inner = 1 + hi

        def own(k):
            rs_end(s0, k).wait_recv()
            solve_items(k, part[s0, k] + rec_x[s0, k])
            ag(s0, k, inner).start()

        def take(s):
            def body(k):
                ag(s, k, inner).wait_recv()

            return body

        gather()
        each(own)
        for s in (s1, s2, s3):
            each(take(s))
        sent(part, rs_sem, 3)
        sent(vout.at[:, :blk], ag_sem, 1)

    @pl.when(is_mid == 1)
    def _():
        def outer_to_cross(s):
            def body(k):
                rs_out(s, k).wait_recv()
                part[s, k] = part[s, k] + rec_e[s, k]
                rs_cross(s, k).start()

            return body

        def cross_to_end(k):
            rs_cross(s0, k).wait_recv()
            part[s0, k] = part[s0, k] + rec_x[s0, k]
            rs_end(s0, k).start()

        def own(k):
            rs_out(s1, k).wait_recv()
            rs_cross(s1, k).wait_recv()
            solve_items(k, part[s1, k] + (rec_e[s1, k] + rec_x[s1, k]))
            ag(s1, k, cross).start()
            ag(s1, k, end).start()

        def relay(s, row):
            def body(k):
                ag(s, k, row).wait_recv()
                ag(s, k, row).start()

            return body

        def out(k):
            outer_to_cross(s3)(k)
            outer_to_cross(s2)(k)

        work = (
            (OUT_AT, out), (END_AT, cross_to_end), (OWN_AT, own),
            (NEAR_AT, relay(s2, end)), (OUTER_AT, relay(s0, cross)), (FAR_AT, relay(s3, end)),
        )

        def step(t):
            @pl.when(t == OWN_AT[0])
            def _():
                gather()

            for (at, every), body in work:
                k = (t - at + every * nc) // every - nc

                @pl.when((k >= 0) & (k < nc) & (at + k * every == t))
                def _():
                    body(k)

        each(step, max(at + every * (nc - 1) for (at, every), _ in work) + 1)
        sent(part, rs_sem, 3)
        for _ in range(5):
            sent(vout.at[:, :blk], ag_sem, 1)

    sent(wg, ws_sem, 3)
    sent(mown, ms_sem, 3)
    sent(ar.at[:, :3], as_sem, None)


def finish_kernel(u_in, v_in, u_out, v_out, sem):
    copies = [pltpu.make_async_copy(v_in, v_out, sem.at[0]), pltpu.make_async_copy(u_in, u_out, sem.at[1])]
    for copy in copies:
        copy.start()
    for copy in copies:
        copy.wait()


def solution(mesh):
    row_size = mesh.shape["row"]
    col_size = mesh.shape["col"]
    assert row_size == 4 and col_size == 4
    grid_spec = P(("part", "row"), "col")
    user_spec = P(("part", "row"), None)
    item_spec = P(("part", "col"), None)

    def local_step(ratings, mask, user_blk, item_blk):
        users, items = ratings.shape
        rank = user_blk.shape[1]
        blk = items // row_size
        width = blk // CHUNKS
        ridge_u, ridge_i = RIDGE_WEIGHT * (items * col_size), RIDGE_WEIGHT * (users * row_size)
        vmem, any_space = pl.BlockSpec(memory_space=pltpu.VMEM), pl.BlockSpec(memory_space=pl.ANY)
        dma = pltpu.SemaphoreType.DMA
        sums = pltpu.VMEM((4, CHUNKS, rank, width), F32)
        user_new, item_new = pl.pallas_call(
            functools.partial(kernel, ridge_u, ridge_i),
            out_shape=(pltpu.VMEM((rank, users), F32), pltpu.VMEM((rank, items), F32)),
            in_specs=[any_space, any_space, vmem, any_space],
            out_specs=(vmem, vmem),
            scratch_shapes=[
                pltpu.VMEM((4, users, blk), jnp.int32),
                pltpu.VMEM((4, users, blk), F32),
                pltpu.VMEM((4, rank, blk), F32),
                pltpu.VMEM((4, rank, blk), BF),
                pltpu.VMEM((4, CHUNKS, users, width), BF),
                pltpu.VMEM((4, CHUNKS, users, width), BF),
                pltpu.VMEM((CG_STEPS + 1, 4, rank, users), F32),
                pltpu.VMEM((4, rank, users), BF),
                pltpu.VMEM((4 * users, rank), BF),
                pltpu.VMEM((rank, 4 * users), BF),
                sums, sums, sums,
                dma((3, 4)), dma, dma((4,)), dma, dma((CG_STEPS + 1, 4)), dma, dma((4,)),
                dma, dma((4, CHUNKS)), dma((4, CHUNKS)), dma, dma((4, CHUNKS)),
            ],
            compiler_params=pltpu.CompilerParams(
                collective_id=0, has_side_effects=True, vmem_limit_bytes=56 * 2**20),
            name="als_sweep",
        )(ratings, mask, user_blk.T, item_blk.T)
        user_new, item_new = pl.pallas_call(
            finish_kernel,
            out_shape=(jax.ShapeDtypeStruct((rank, users), F32), jax.ShapeDtypeStruct((rank, items), F32)),
            in_specs=[vmem, vmem],
            out_specs=(any_space, any_space),
            scratch_shapes=[dma((2,))],
            name="write_out",
        )(*(pltpu.with_memory_space_constraint(x, pltpu.VMEM) for x in (user_new, item_new)))
        return user_new.T, item_new.T

    return jax.shard_map(local_step, mesh=mesh, in_specs=(grid_spec, grid_spec, user_spec, item_spec), out_specs=(user_spec, item_spec), check_vma=False)
```

```python
import functools

import jax
import jax.numpy as jnp
from jax import lax
from jax.experimental import pallas as pl
from jax.experimental.pallas import tpu as pltpu
from jax.sharding import PartitionSpec as P

CG_STEPS = 4
RIDGE_WEIGHT = 0.0005
CHUNKS = 8
FAR_SUM, NEAR_SUM, END_SUM, NEAR_RES, END_RES, FAR_RES = range(6)
RELAYS = (
    ((FAR_SUM, 0), (NEAR_SUM, 0), (FAR_SUM, 1), (NEAR_SUM, 1), (FAR_SUM, 2), (END_SUM, 0), (NEAR_SUM, 2)),
    ((END_SUM, 1), (FAR_SUM, 3)),
    ((NEAR_SUM, 3), (END_SUM, 2)),
    ((FAR_SUM, 4), (NEAR_RES, 0), (NEAR_SUM, 4), (END_SUM, 3), (NEAR_RES, 1), (FAR_SUM, 5)),
    ((NEAR_SUM, 5), (NEAR_RES, 2), (END_SUM, 4), (FAR_SUM, 6)),
    ((NEAR_SUM, 6), (END_SUM, 5), (NEAR_RES, 3), (FAR_SUM, 7)),
    ((NEAR_SUM, 7), (END_SUM, 6), (NEAR_RES, 4), (END_RES, 0)),
    ((END_SUM, 7), (END_RES, 1), (END_RES, 2), (NEAR_RES, 5), (END_RES, 3)),
    ((END_RES, 4), (FAR_RES, 0), (END_RES, 5), (NEAR_RES, 6), (END_RES, 6), (FAR_RES, 1), (FAR_RES, 2), (FAR_RES, 3), (END_RES, 7), (NEAR_RES, 7), (FAR_RES, 4), (FAR_RES, 5), (FAR_RES, 6), (FAR_RES, 7)),
)
BF, F32 = jnp.bfloat16, jnp.float32
MESH = pl.DeviceIdType.MESH


def mm(a, b, contract_a, contract_b):
    return lax.dot_general(a, b, (((contract_a,), (contract_b,)), ((), ())), preferred_element_type=F32)


def col_sum(a, b):
    return jnp.sum(a * b, axis=0, keepdims=True)


def cg_steps(apply_a, start, residual):
    direction = residual
    estimate = start
    res_sq = col_sum(residual, residual)
    for cg_step in range(CG_STEPS):
        gram_dir = apply_a(direction)
        step_size = res_sq / col_sum(direction, gram_dir)
        estimate = estimate + step_size * direction
        if cg_step + 1 < CG_STEPS:
            residual = residual - step_size * gram_dir
            new_sq = col_sum(residual, residual)
            direction = residual + (new_sq / res_sq) * direction
            res_sq = new_sq
    return estimate


def kernel(
    ridge_u, ridge_i,
    r_hbm, m_hbm, w0_ref, v0_hbm,
    u_out, vout,
    mint, rbuf, v0b, fb, mown, mrecv, ar, wg, wrow, wcol, part, rec_e, rec_x,
    ld_sem, ms_sem, mr_sem, as_sem, arr_sem, ws_sem, wr_sem, rs_sem, chunk_sem, across_sem, ag_sem, near_sem, far_sem,
):
    z = lax.axis_index("row")
    c = lax.axis_index("col")
    blk = mint.shape[2]
    nc, width = part.shape[1], part.shape[3]
    hi = z // 2
    is_mid = lax.rem(z + hi, 2)

    def row_of(mirrored):
        return mirrored + hi * (3 - 2 * mirrored)

    def to_row(src, dst, send, recv, row):
        return pltpu.make_async_remote_copy(
            src_ref=src, dst_ref=dst, send_sem=send, recv_sem=recv, device_id={"row": row}, device_id_type=MESH)

    def sent(buf, sem, n):
        src = buf if n is None else buf.at[:n]
        to_row(src, src, sem, sem, z).wait_send()

    cross, end = 3 - z, 3 * hi
    order = (2 - hi, 3 - 3 * hi, is_mid * end + (1 - is_mid) * (1 + hi), z)

    def load(hbm, buf, kind, s):
        return pltpu.make_async_copy(
            hbm.at[:, pl.ds(pl.multiple_of(s * blk, blk), blk)], buf.at[s], ld_sem.at[kind, s])

    barrier = pltpu.get_barrier_semaphore()
    load(m_hbm, mint, 0, order[0]).start()

    def tell(sem, row):
        pl.semaphore_signal(sem, inc=1, device_id={"row": row}, device_id_type=MESH)

    @pl.when(is_mid == 1)
    def _():
        tell(barrier, cross)
        tell(barrier, end)

    @pl.when(is_mid == 0)
    def _():
        tell(barrier, 1 + hi)

    for off in range(1, 4):
        pl.semaphore_signal(barrier, inc=1, device_id={"col": lax.rem(c + off, 4)}, device_id_type=MESH)
    load(v0_hbm, v0b, 1, order[0]).start()
    load(r_hbm, rbuf, 2, order[0]).start()
    for s in order[1:]:
        load(m_hbm, mint, 0, s).start()
        load(v0_hbm, v0b, 1, s).start()
        load(r_hbm, rbuf, 2, s).start()

    def observed(s, k, scores):
        cols = pl.ds(pl.multiple_of(k * width, width), width)
        return jnp.where(mint[s, :, cols] > 0, rbuf[s, :, cols] - scores, 0.0).astype(BF)

    def send_mask(s):
        to_row(mown.at[s], mrecv.at[z], ms_sem, mr_sem.at[z], s).start()

    w0 = w0_ref[...]
    rows0 = w0.T.astype(BF)
    first = jnp.zeros((w0.shape[1], w0.shape[0]), F32)
    for j, s in enumerate(order):
        load(m_hbm, mint, 0, s).wait()
        for k in range(nc):
            m = mint[s, :, k * width:(k + 1) * width].astype(F32).astype(BF)
            mown[s, k] = m
            if j == 3:
                mrecv[z, k] = m
        if j == 0:
            pl.semaphore_wait(barrier, 4 + is_mid)

            @pl.when(is_mid == 1)
            def _():
                tell(far_sem, cross)
                tell(near_sem, end)

            @pl.when(is_mid == 0)
            def _():
                pl.semaphore_wait(near_sem, 1)

        if j == 1:
            pl.semaphore_wait(far_sem, 1)

            @pl.when(is_mid == 1)
            def _():
                tell(far_sem, end)

        if j < 3:
            send_mask(s)
        load(v0_hbm, v0b, 1, s).wait()
        load(r_hbm, rbuf, 2, s).wait()
        for k in range(nc):
            cols = slice(k * width, (k + 1) * width)
            f = v0b[s, :, cols].astype(BF)
            fb[s, :, cols] = f
            first = first + mm(observed(s, k, mm(rows0, f, 1, 0)), f, 1, 1)

    def user_product(x):
        rows = x.T.astype(BF)
        acc = jnp.zeros((x.shape[1], x.shape[0]), F32)
        for s in range(4):
            for k in range(0, nc, 2):
                f = fb[s, :, k * width:(k + 2) * width]
                mask = jnp.concatenate([mown[s, k], mown[s, k + 1]], axis=1)
                acc = acc + mm(mask * mm(rows, f, 1, 0).astype(BF), f, 1, 1)
        return acc.T

    def to_col(rnd, off):
        peer = lax.rem(c + off, 4)
        return pltpu.make_async_remote_copy(
            src_ref=ar.at[rnd, c], dst_ref=ar.at[rnd, c], send_sem=as_sem, recv_sem=arr_sem.at[lax.rem(rnd, 2), c],
            device_id={"col": peer}, device_id_type=MESH)

    def from_col(rnd, off):
        peer = lax.rem(c + off, 4)
        return pltpu.make_async_remote_copy(
            src_ref=ar.at[rnd, peer], dst_ref=ar.at[rnd, peer], send_sem=as_sem,
            recv_sem=arr_sem.at[lax.rem(rnd, 2), peer], device_id={"col": peer}, device_id_type=MESH)

    def sum_cols(rnd, x):
        ar[rnd, c] = x
        for off in range(1, 4):
            to_col(rnd, off).start()
        for off in range(1, 4):
            from_col(rnd, off).wait_recv()
        return (ar[rnd, 0] + ar[rnd, 1]) + (ar[rnd, 2] + ar[rnd, 3])

    res = sum_cols(0, first.T) - ridge_u * w0

    def user_step(i, state):
        x, r, p, res_sq = state

        q = sum_cols(i + 1, user_product(p)) + ridge_u * p
        step_size = res_sq / col_sum(p, q)
        x = x + step_size * p
        r = r - step_size * q
        new_sq = col_sum(r, r)
        p = r + (new_sq / res_sq) * p
        return x, r, p, new_sq

    w1 = lax.fori_loop(0, CG_STEPS, user_step, (w0, res, res, col_sum(res, res)))[0]
    u_out[...] = w1

    def give(src_row, row):
        return to_row(wg.at[src_row], wg.at[src_row], ws_sem, wr_sem.at[src_row], row)

    wg[z] = w1.astype(BF)

    @pl.when(is_mid == 0)
    def _():
        give(z, 1 + hi).start()

    @pl.when(is_mid == 1)
    def _():
        give(z, cross).start()
        give(z, end).start()

    own_rows = w1.T.astype(BF)
    own_cols = w1.astype(BF)

    def rs_out(s, k):
        return to_row(part.at[s, k], rec_e.at[s, k], rs_sem, chunk_sem.at[s, k], 1 + hi)

    def rs_cross(s, k, sem):
        return to_row(part.at[s, k], rec_x.at[s, k], rs_sem, sem, cross)

    def rs_end(s, k):
        return to_row(part.at[s, k], rec_x.at[s, k], rs_sem, chunk_sem.at[s, k], end)

    def each(body, n=nc):
        def step(k, carry):
            body(k)
            return carry

        lax.fori_loop(0, n, step, 0)

    def outer_first(j):
        return row_of(3 - j)

    def partial_sums(k):
        for j in range(4):
            s = outer_first(j)
            f = fb[s, :, pl.ds(pl.multiple_of(k * width, width), width)]
            part[s, k] = mm(own_cols, observed(s, k, mm(own_rows, f, 1, 0)), 1, 0)

        @pl.when(is_mid == 0)
        def _():
            for j in range(3):
                rs_out(outer_first(j), k).start()

    each(partial_sums)

    def gather():
        for off in range(1, 4):
            peer = lax.rem(z + off, 4)
            @pl.when((is_mid == 0) | (peer != end))
            def _():
                give(peer, end).wait_recv()

            @pl.when((is_mid == 1) & (peer != end))
            def _():
                give(peer, end).start()

            to_row(mown.at[peer], mrecv.at[peer], ms_sem, mr_sem.at[peer], peer).wait_recv()
        users = own_rows.shape[0]
        for s in range(4):
            wrow[s * users:(s + 1) * users] = wg[s].astype(F32).T.astype(BF)
            wcol[:, s * users:(s + 1) * users] = wg[s]

    def cols_of(s, k):
        return pl.ds(pl.multiple_of(s * blk + k * width, width), width)

    def solve_items(k, residual):
        start = v0b[z, :, pl.ds(pl.multiple_of(k * width, width), width)]

        def apply_a(p):
            masked = jnp.concatenate([mrecv[t, k] for t in range(4)], axis=0)
            masked = masked * mm(wrow[...], p.astype(BF), 1, 0).astype(BF)
            return mm(wcol[...], masked, 1, 0) + ridge_i * p

        vout[:, cols_of(z, k)] = cg_steps(apply_a, start, residual - ridge_i * start)

    def ag(s, k, row):
        chunk = vout.at[:, cols_of(s, k)]
        return to_row(chunk, chunk, ag_sem, chunk_sem.at[s, k], row)

    s0, s1, s2, s3 = (row_of(m) for m in range(4))

    @pl.when(is_mid == 0)
    def _():
        inner = 1 + hi

        def own(k):
            rs_end(s0, k).wait_recv()
            solve_items(k, part[s0, k] + rec_x[s0, k])
            ag(s0, k, inner).start()

        def take(s):
            def body(k):
                ag(s, k, inner).wait_recv()

            return body

        gather()
        each(own)
        for s in (s1, s2, s3):
            each(take(s))
        sent(wg, ws_sem, 1)
        sent(part, rs_sem, 3)
        sent(vout.at[:, :blk], ag_sem, None)

    @pl.when(is_mid == 1)
    def _():
        def outer_to_cross(s, sem):
            def body(k):
                rs_out(s, k).wait_recv()
                part[s, k] = part[s, k] + rec_e[s, k]
                rs_cross(s, k, sem(k)).start()

            return body

        def cross_to_end(k):
            rs_cross(s0, k, chunk_sem.at[s0, k]).wait_recv()
            part[s0, k] = part[s0, k] + rec_x[s0, k]
            rs_end(s0, k).start()

        def own(k):
            rs_out(s1, k).wait_recv()
            rs_cross(s1, k, across_sem.at[k]).wait_recv()
            solve_items(k, part[s1, k] + (rec_e[s1, k] + rec_x[s1, k]))
            ag(s1, k, cross).start()
            ag(s1, k, end).start()

        def relay(s, row):
            def body(k):
                ag(s, k, row).wait_recv()
                ag(s, k, row).start()

            return body

        relays = (
            outer_to_cross(s3, lambda k: chunk_sem.at[s3, k]), outer_to_cross(s2, lambda k: across_sem.at[k]), cross_to_end, relay(s2, end), relay(s0, cross), relay(s3, end),
        )
        give(end, cross).wait_recv()
        give(end, cross).start()
        for kind, k in RELAYS[0]:
            relays[kind](k)
        gather()

        def step(j):
            own(j)
            for i in range(nc):
                @pl.when(j == i)
                def _():
                    for kind, k in RELAYS[i + 1]:
                        relays[kind](k)

        each(step)
        sent(wg, ws_sem, 4)
        sent(wg, ws_sem, 1)
        sent(part, rs_sem, 3)
        for _ in range(5):
            sent(vout.at[:, :blk], ag_sem, None)

    sent(mown, ms_sem, 3)
    sent(ar.at[:, :3], as_sem, None)


def finish_kernel(u_in, v_in, u_out, v_out, sem):
    copies = [pltpu.make_async_copy(v_in, v_out, sem.at[0]), pltpu.make_async_copy(u_in, u_out, sem.at[1])]
    for copy in copies:
        copy.start()
    for copy in copies:
        copy.wait()


def solution(mesh):
    row_size = mesh.shape["row"]
    col_size = mesh.shape["col"]
    assert row_size == 4 and col_size == 4
    grid_spec = P(("part", "row"), "col")
    user_spec = P(("part", "row"), None)
    item_spec = P(("part", "col"), None)

    def local_step(ratings, mask, user_blk, item_blk):
        users, items = ratings.shape
        rank = user_blk.shape[1]
        blk = items // row_size
        width = blk // CHUNKS
        ridge_u, ridge_i = RIDGE_WEIGHT * (items * col_size), RIDGE_WEIGHT * (users * row_size)
        vmem, any_space = pl.BlockSpec(memory_space=pltpu.VMEM), pl.BlockSpec(memory_space=pl.ANY)
        dma = pltpu.SemaphoreType.DMA
        sums = pltpu.VMEM((4, CHUNKS, rank, width), F32)
        user_new, item_new = pl.pallas_call(
            functools.partial(kernel, ridge_u, ridge_i),
            out_shape=(pltpu.VMEM((rank, users), F32), pltpu.VMEM((rank, items), F32)),
            in_specs=[any_space, any_space, vmem, any_space],
            out_specs=(vmem, vmem),
            scratch_shapes=[
                pltpu.VMEM((4, users, blk), jnp.int32),
                pltpu.VMEM((4, users, blk), F32),
                pltpu.VMEM((4, rank, blk), F32),
                pltpu.VMEM((4, rank, blk), BF),
                pltpu.VMEM((4, CHUNKS, users, width), BF),
                pltpu.VMEM((4, CHUNKS, users, width), BF),
                pltpu.VMEM((CG_STEPS + 1, 4, rank, users), F32),
                pltpu.VMEM((4, rank, users), BF),
                pltpu.VMEM((4 * users, rank), BF),
                pltpu.VMEM((rank, 4 * users), BF),
                sums, sums, sums,
                dma((3, 4)), dma, dma((4,)), dma, dma((2, 4)), dma, dma((4,)),
                dma, dma((4, CHUNKS)), dma((CHUNKS,)), dma,
                pltpu.SemaphoreType.REGULAR, pltpu.SemaphoreType.REGULAR,
            ],
            compiler_params=pltpu.CompilerParams(
                collective_id=0, has_side_effects=True, vmem_limit_bytes=56 * 2**20),
            name="als_sweep",
        )(ratings, mask, user_blk.T, item_blk.T)
        user_new, item_new = pl.pallas_call(
            finish_kernel,
            out_shape=(jax.ShapeDtypeStruct((rank, users), F32), jax.ShapeDtypeStruct((rank, items), F32)),
            in_specs=[vmem, vmem],
            out_specs=(any_space, any_space),
            scratch_shapes=[dma((2,))],
            name="write_out",
        )(*(pltpu.with_memory_space_constraint(x, pltpu.VMEM) for x in (user_new, item_new)))
        return user_new.T, item_new.T

    return jax.shard_map(local_step, mesh=mesh, in_specs=(grid_spec, grid_spec, user_spec, item_spec), out_specs=(user_spec, item_spec), check_vma=False)
```

```python
import functools

import jax
import jax.numpy as jnp
from jax import lax
from jax.experimental import pallas as pl
from jax.experimental.pallas import tpu as pltpu
from jax.sharding import PartitionSpec as P

CG_STEPS = 4
RIDGE_WEIGHT = 0.0005
CHUNKS = 8
FAR_SUM, NEAR_SUM, END_SUM, NEAR_RES, END_RES, FAR_RES = range(6)
RELAYS = (
    ((FAR_SUM, 0), (NEAR_SUM, 0), (FAR_SUM, 1), (NEAR_SUM, 1), (FAR_SUM, 2), (END_SUM, 0), (NEAR_SUM, 2)),
    ((END_SUM, 1), (FAR_SUM, 3)),
    ((NEAR_SUM, 3), (END_SUM, 2)),
    ((FAR_SUM, 4), (NEAR_RES, 0), (NEAR_SUM, 4), (END_SUM, 3), (NEAR_RES, 1), (FAR_SUM, 5)),
    ((NEAR_SUM, 5), (NEAR_RES, 2), (END_SUM, 4), (FAR_SUM, 6)),
    ((NEAR_SUM, 6), (END_SUM, 5), (NEAR_RES, 3), (FAR_SUM, 7)),
    ((NEAR_SUM, 7), (END_SUM, 6), (NEAR_RES, 4), (END_RES, 0)),
    ((END_SUM, 7), (END_RES, 1), (END_RES, 2), (NEAR_RES, 5), (END_RES, 3)),
    ((END_RES, 4), (FAR_RES, 0), (END_RES, 5), (NEAR_RES, 6), (END_RES, 6), (FAR_RES, 1), (FAR_RES, 2), (FAR_RES, 3), (END_RES, 7), (NEAR_RES, 7), (FAR_RES, 4), (FAR_RES, 5), (FAR_RES, 6), (FAR_RES, 7)),
)
HOLD = 3
BF, F32 = jnp.bfloat16, jnp.float32
MESH = pl.DeviceIdType.MESH


def mm(a, b, contract_a, contract_b):
    return lax.dot_general(a, b, (((contract_a,), (contract_b,)), ((), ())), preferred_element_type=F32)


def col_sum(a, b):
    return jnp.sum(a * b, axis=0, keepdims=True)


def cg_steps(apply_a, start, residual):
    direction = residual
    estimate = start
    res_sq = col_sum(residual, residual)
    for cg_step in range(CG_STEPS):
        gram_dir = apply_a(direction)
        step_size = res_sq / col_sum(direction, gram_dir)
        estimate = estimate + step_size * direction
        if cg_step + 1 < CG_STEPS:
            residual = residual - step_size * gram_dir
            new_sq = col_sum(residual, residual)
            direction = residual + (new_sq / res_sq) * direction
            res_sq = new_sq
    return estimate


def kernel(
    ridge_u, ridge_i,
    r_hbm, m_hbm, w0_ref, v0_hbm,
    u_out, vout,
    mint, rbuf, v0b, fb, mown, mrecv, ar, wg, wrow, wcol, part, rec_e, rec_x,
    ld_sem, v_sem, r_sem, ms_sem, mr_sem, as_sem, arr_sem, ws_sem, wr_sem, rs_sem, chunk_sem, across_sem, ag_sem, near_sem, far_sem,
):
    z = lax.axis_index("row")
    c = lax.axis_index("col")
    blk = mint.shape[2]
    nc, width = part.shape[1], part.shape[3]
    hi = z // 2
    is_mid = lax.rem(z + hi, 2)

    def row_of(mirrored):
        return mirrored + hi * (3 - 2 * mirrored)

    def to_row(src, dst, send, recv, row):
        return pltpu.make_async_remote_copy(
            src_ref=src, dst_ref=dst, send_sem=send, recv_sem=recv, device_id={"row": row}, device_id_type=MESH)

    def sent(buf, sem, n):
        src = buf if n is None else buf.at[:n]
        to_row(src, src, sem, sem, z).wait_send()

    cross, end = 3 - z, 3 * hi
    order = (2 - hi, 3 - 3 * hi, is_mid * end + (1 - is_mid) * (1 + hi), z)

    def load(hbm, buf, s, sem):
        return pltpu.make_async_copy(hbm.at[:, pl.ds(pl.multiple_of(s * blk, blk), blk)], buf.at[s], sem)

    barrier = pltpu.get_barrier_semaphore()
    load(m_hbm, mint, order[0], ld_sem.at[0]).start()

    def tell(sem, row):
        pl.semaphore_signal(sem, inc=1, device_id={"row": row}, device_id_type=MESH)

    @pl.when(is_mid == 1)
    def _():
        tell(barrier, cross)
        tell(barrier, end)

    @pl.when(is_mid == 0)
    def _():
        tell(barrier, 1 + hi)

    for off in range(1, 4):
        pl.semaphore_signal(barrier, inc=1, device_id={"col": lax.rem(c + off, 4)}, device_id_type=MESH)
    def observed(s, k, scores):
        cols = pl.ds(pl.multiple_of(k * width, width), width)
        return jnp.where(mint[s, :, cols] > 0, rbuf[s, :, cols] - scores, 0.0).astype(BF)

    def send_mask(s):
        to_row(mown.at[s], mrecv.at[z], ms_sem, mr_sem.at[z], s).start()

    w0 = w0_ref[...]
    rows0 = w0.T.astype(BF)
    first = jnp.zeros((w0.shape[1], w0.shape[0]), F32)
    for j, s in enumerate(order):
        load(m_hbm, mint, s, ld_sem.at[j]).wait()
        for k in range(nc):
            m = mint[s, :, k * width:(k + 1) * width].astype(F32).astype(BF)
            mown[s, k] = m
            if j == 3:
                mrecv[z, k] = m
        if j == 0:
            pl.semaphore_wait(barrier, 4 + is_mid)

            @pl.when(is_mid == 1)
            def _():
                tell(far_sem, cross)
                tell(near_sem, end)

            @pl.when(is_mid == 0)
            def _():
                pl.semaphore_wait(near_sem, 1)

        if j == 1:
            pl.semaphore_wait(far_sem, 1)

            @pl.when(is_mid == 1)
            def _():
                tell(far_sem, end)

        if j < 3:
            send_mask(s)
        if j == 0:
            for i, other in enumerate(order):
                if i:
                    load(m_hbm, mint, other, ld_sem.at[i]).start()
                load(v0_hbm, v0b, other, v_sem).start()
                load(r_hbm, rbuf, other, r_sem).start()
            pltpu.make_async_copy(v0b, v0b, v_sem).wait()
            pltpu.make_async_copy(rbuf, rbuf, r_sem).wait()
        for k in range(nc):
            cols = slice(k * width, (k + 1) * width)
            f = v0b[s, :, cols].astype(BF)
            fb[s, :, cols] = f
            first = first + mm(observed(s, k, mm(rows0, f, 1, 0)), f, 1, 1)

    def user_product(x):
        rows = x.T.astype(BF)
        acc = jnp.zeros((x.shape[1], x.shape[0]), F32)
        for s in range(4):
            for k in range(0, nc, 2):
                f = fb[s, :, k * width:(k + 2) * width]
                mask = jnp.concatenate([mown[s, k], mown[s, k + 1]], axis=1)
                acc = acc + mm(mask * mm(rows, f, 1, 0).astype(BF), f, 1, 1)
        return acc.T

    def to_col(rnd, off):
        peer = lax.rem(c + off, 4)
        return pltpu.make_async_remote_copy(
            src_ref=ar.at[rnd, c], dst_ref=ar.at[rnd, c], send_sem=as_sem, recv_sem=arr_sem.at[lax.rem(rnd, 2), c],
            device_id={"col": peer}, device_id_type=MESH)

    def from_col(rnd, off):
        peer = lax.rem(c + off, 4)
        return pltpu.make_async_remote_copy(
            src_ref=ar.at[rnd, peer], dst_ref=ar.at[rnd, peer], send_sem=as_sem,
            recv_sem=arr_sem.at[lax.rem(rnd, 2), peer], device_id={"col": peer}, device_id_type=MESH)

    def sum_cols(rnd, x):
        ar[rnd, c] = x
        for off in range(1, 4):
            to_col(rnd, off).start()
        for off in range(1, 4):
            from_col(rnd, off).wait_recv()
        return (ar[rnd, 0] + ar[rnd, 1]) + (ar[rnd, 2] + ar[rnd, 3])

    res = sum_cols(0, first.T) - ridge_u * w0

    def user_step(i, state):
        x, r, p, res_sq = state

        q = sum_cols(i + 1, user_product(p)) + ridge_u * p
        step_size = res_sq / col_sum(p, q)
        x = x + step_size * p
        r = r - step_size * q
        new_sq = col_sum(r, r)
        p = r + (new_sq / res_sq) * p
        return x, r, p, new_sq

    w1 = lax.fori_loop(0, CG_STEPS, user_step, (w0, res, res, col_sum(res, res)))[0]
    u_out[...] = w1

    def give(src_row, row):
        return to_row(wg.at[src_row], wg.at[src_row], ws_sem, wr_sem.at[src_row], row)

    wg[z] = w1.astype(BF)

    @pl.when(is_mid == 0)
    def _():
        give(z, 1 + hi).start()

    @pl.when(is_mid == 1)
    def _():
        give(z, cross).start()
        give(z, end).start()

    own_rows = w1.T.astype(BF)
    own_cols = w1.astype(BF)

    def rs_out(s, k):
        return to_row(part.at[s, k], rec_e.at[s, k], rs_sem, chunk_sem.at[s, k], 1 + hi)

    def rs_cross(s, k, sem):
        return to_row(part.at[s, k], rec_x.at[s, k], rs_sem, sem, cross)

    def rs_end(s, k):
        return to_row(part.at[s, k], rec_x.at[s, k], rs_sem, chunk_sem.at[s, k], end)

    def each(body, n=nc):
        def step(k, carry):
            body(k)
            return carry

        lax.fori_loop(0, n, step, 0)

    def outer_first(j):
        return row_of(3 - j)

    def partial_sums(k):
        for j in range(4):
            s = outer_first(j)
            f = fb[s, :, pl.ds(pl.multiple_of(k * width, width), width)]
            part[s, k] = mm(own_cols, observed(s, k, mm(own_rows, f, 1, 0)), 1, 0)

        @pl.when(is_mid == 0)
        def _():
            for j in range(3):
                rs_out(outer_first(j), k).start()

    each(partial_sums)

    def gather():
        for off in range(1, 4):
            peer = lax.rem(z + off, 4)
            @pl.when((is_mid == 0) | (peer != end))
            def _():
                give(peer, end).wait_recv()

            @pl.when((is_mid == 1) & (peer != end))
            def _():
                give(peer, end).start()

            to_row(mown.at[peer], mrecv.at[peer], ms_sem, mr_sem.at[peer], peer).wait_recv()
        users = own_rows.shape[0]
        for s in range(4):
            wrow[s * users:(s + 1) * users] = wg[s].astype(F32).T.astype(BF)
            wcol[:, s * users:(s + 1) * users] = wg[s]

    def cols_of(s, k):
        return pl.ds(pl.multiple_of(s * blk + k * width, width), width)

    def solve_items(k, residual):
        start = v0b[z, :, pl.ds(pl.multiple_of(k * width, width), width)]

        def apply_a(p):
            pb = p.astype(BF)
            users = wrow.shape[0] // 2
            halves = []
            for i in range(2):
                mask = jnp.concatenate([mrecv[2 * i, k], mrecv[2 * i + 1, k]], axis=0)
                halves.append(mask * mm(wrow[i * users:(i + 1) * users], pb, 1, 0).astype(BF))
            return mm(wcol[...], jnp.concatenate(halves, axis=0), 1, 0) + ridge_i * p

        vout[:, cols_of(z, k)] = cg_steps(apply_a, start, residual - ridge_i * start)

    def ag(s, k, row):
        chunk = vout.at[:, cols_of(s, k)]
        return to_row(chunk, chunk, ag_sem, chunk_sem.at[s, k], row)

    s0, s1, s2, s3 = (row_of(m) for m in range(4))

    @pl.when(is_mid == 0)
    def _():
        inner = 1 + hi

        def own(k):
            rs_end(s0, k).wait_recv()
            solve_items(k, part[s0, k] + rec_x[s0, k])
            ag(s0, k, inner).start()

        def take(s):
            def body(k):
                ag(s, k, inner).wait_recv()

            return body

        gather()
        each(own)
        for s in (s1, s2, s3):
            each(take(s))
        sent(wg, ws_sem, 1)
        sent(part, rs_sem, 3)
        sent(vout.at[:, :blk], ag_sem, None)

    @pl.when(is_mid == 1)
    def _():
        def outer_to_cross(s, sem):
            def body(k):
                rs_out(s, k).wait_recv()
                part[s, k] = part[s, k] + rec_e[s, k]
                rs_cross(s, k, sem(k)).start()

            return body

        def cross_to_end(k):
            rs_cross(s0, k, chunk_sem.at[s0, k]).wait_recv()
            part[s0, k] = part[s0, k] + rec_x[s0, k]
            rs_end(s0, k).start()

        def own(k):
            rs_out(s1, k).wait_recv()
            rs_cross(s1, k, across_sem.at[k]).wait_recv()
            solve_items(k, part[s1, k] + (rec_e[s1, k] + rec_x[s1, k]))
            ag(s1, k, cross).start()
            ag(s1, k, end).start()

        def relay(s, row):
            def body(k):
                ag(s, k, row).wait_recv()
                ag(s, k, row).start()

            return body

        def held_relay(s, row):
            def body(k):
                ag(s, k, row).wait_recv()

                @pl.when(lax.rem(c, 2) == 0)
                def _():
                    ag(s, k, row).start()

                @pl.when(lax.rem(c, 2) == 1)
                def _():
                    if k >= HOLD:
                        ag(s, k - HOLD, row).start()
                    if k == nc - 1:
                        for i in range(nc - HOLD, nc):
                            ag(s, i, row).start()

            return body

        relays = (
            outer_to_cross(s3, lambda k: chunk_sem.at[s3, k]), outer_to_cross(s2, lambda k: across_sem.at[k]), cross_to_end, relay(s2, end), held_relay(s0, cross), relay(s3, end),
        )
        give(end, cross).wait_recv()
        give(end, cross).start()
        for kind, k in RELAYS[0]:
            relays[kind](k)
        gather()

        def step(j):
            own(j)
            for i in range(nc):
                @pl.when(j == i)
                def _():
                    for kind, k in RELAYS[i + 1]:
                        relays[kind](k)

        each(step)
        sent(wg, ws_sem, 4)
        sent(wg, ws_sem, 1)
        sent(part, rs_sem, 3)
        for _ in range(5):
            sent(vout.at[:, :blk], ag_sem, None)

    sent(mown, ms_sem, 3)
    sent(ar.at[:, :3], as_sem, None)


def finish_kernel(u_in, v_in, u_out, v_out, sem):
    copies = [pltpu.make_async_copy(v_in, v_out, sem.at[0]), pltpu.make_async_copy(u_in, u_out, sem.at[1])]
    for copy in copies:
        copy.start()
    for copy in copies:
        copy.wait()


def solution(mesh):
    row_size = mesh.shape["row"]
    col_size = mesh.shape["col"]
    assert row_size == 4 and col_size == 4
    grid_spec = P(("part", "row"), "col")
    user_spec = P(("part", "row"), None)
    item_spec = P(("part", "col"), None)

    def local_step(ratings, mask, user_blk, item_blk):
        users, items = ratings.shape
        rank = user_blk.shape[1]
        blk = items // row_size
        width = blk // CHUNKS
        ridge_u, ridge_i = RIDGE_WEIGHT * (items * col_size), RIDGE_WEIGHT * (users * row_size)
        vmem, any_space = pl.BlockSpec(memory_space=pltpu.VMEM), pl.BlockSpec(memory_space=pl.ANY)
        dma = pltpu.SemaphoreType.DMA
        sums = pltpu.VMEM((4, CHUNKS, rank, width), F32)
        user_new, item_new = pl.pallas_call(
            functools.partial(kernel, ridge_u, ridge_i),
            out_shape=(pltpu.VMEM((rank, users), F32), pltpu.VMEM((rank, items), F32)),
            in_specs=[any_space, any_space, vmem, any_space],
            out_specs=(vmem, vmem),
            scratch_shapes=[
                pltpu.VMEM((4, users, blk), jnp.int32),
                pltpu.VMEM((4, users, blk), F32),
                pltpu.VMEM((4, rank, blk), F32),
                pltpu.VMEM((4, rank, blk), BF),
                pltpu.VMEM((4, CHUNKS, users, width), BF),
                pltpu.VMEM((4, CHUNKS, users, width), BF),
                pltpu.VMEM((CG_STEPS + 1, 4, rank, users), F32),
                pltpu.VMEM((4, rank, users), BF),
                pltpu.VMEM((4 * users, rank), BF),
                pltpu.VMEM((rank, 4 * users), BF),
                sums, sums, sums,
                dma((4,)), dma, dma, dma, dma((4,)), dma, dma((2, 4)), dma, dma((4,)),
                dma, dma((4, CHUNKS)), dma((CHUNKS,)), dma,
                pltpu.SemaphoreType.REGULAR, pltpu.SemaphoreType.REGULAR,
            ],
            compiler_params=pltpu.CompilerParams(
                collective_id=0, has_side_effects=True, vmem_limit_bytes=56 * 2**20),
            name="als_sweep",
        )(ratings, mask, user_blk.T, item_blk.T)
        user_new, item_new = pl.pallas_call(
            finish_kernel,
            out_shape=(jax.ShapeDtypeStruct((rank, users), F32), jax.ShapeDtypeStruct((rank, items), F32)),
            in_specs=[vmem, vmem],
            out_specs=(any_space, any_space),
            scratch_shapes=[dma((2,))],
            name="write_out",
        )(*(pltpu.with_memory_space_constraint(x, pltpu.VMEM) for x in (user_new, item_new)))
        return user_new.T, item_new.T

    return jax.shard_map(local_step, mesh=mesh, in_specs=(grid_spec, grid_spec, user_spec, item_spec), out_specs=(user_spec, item_spec), check_vma=False)
```

```python
import functools

import jax
import jax.numpy as jnp
from jax import lax
from jax.experimental import pallas as pl
from jax.experimental.pallas import tpu as pltpu
from jax.sharding import PartitionSpec as P

CG_STEPS = 4
RIDGE_WEIGHT = 0.0005
CHUNKS = 8
FAR_SUM, NEAR_SUM, END_SUM, NEAR_RES, END_RES, FAR_RES = range(6)
RELAYS = (
    ((FAR_SUM, 0), (NEAR_SUM, 0), (FAR_SUM, 1), (NEAR_SUM, 1), (FAR_SUM, 2), (END_SUM, 0), (NEAR_SUM, 2)),
    ((END_SUM, 1), (FAR_SUM, 3)),
    ((NEAR_SUM, 3), (END_SUM, 2)),
    ((FAR_SUM, 4), (NEAR_RES, 0), (NEAR_SUM, 4), (END_SUM, 3), (NEAR_RES, 1), (FAR_SUM, 5)),
    ((NEAR_SUM, 5), (NEAR_RES, 2), (END_SUM, 4), (FAR_SUM, 6)),
    ((NEAR_SUM, 6), (END_SUM, 5), (NEAR_RES, 3), (FAR_SUM, 7)),
    ((NEAR_SUM, 7), (END_SUM, 6), (NEAR_RES, 4), (END_RES, 0)),
    ((END_SUM, 7), (END_RES, 1), (END_RES, 2), (NEAR_RES, 5), (END_RES, 3)),
    ((END_RES, 4), (FAR_RES, 0), (END_RES, 5), (NEAR_RES, 6), (END_RES, 6), (FAR_RES, 1), (FAR_RES, 2), (FAR_RES, 3), (END_RES, 7), (NEAR_RES, 7), (FAR_RES, 4), (FAR_RES, 5), (FAR_RES, 6), (FAR_RES, 7)),
)
HOLD = 3
BF, F32 = jnp.bfloat16, jnp.float32
MESH = pl.DeviceIdType.MESH


def mm(a, b, contract_a, contract_b):
    return lax.dot_general(a, b, (((contract_a,), (contract_b,)), ((), ())), preferred_element_type=F32)


def col_sum(a, b):
    return jnp.sum(a * b, axis=0, keepdims=True)


def cg_steps(apply_a, start, residual):
    direction = residual
    estimate = start
    res_sq = col_sum(residual, residual)
    for cg_step in range(CG_STEPS):
        gram_dir = apply_a(direction)
        step_size = res_sq / col_sum(direction, gram_dir)
        estimate = estimate + step_size * direction
        if cg_step + 1 < CG_STEPS:
            residual = residual - step_size * gram_dir
            new_sq = col_sum(residual, residual)
            direction = residual + (new_sq / res_sq) * direction
            res_sq = new_sq
    return estimate


def kernel(
    ridge_u, ridge_i,
    r_hbm, m_hbm, w0_hbm, v0_hbm,
    u_out, vout,
    w0_ref, mint, rbuf, v0b, fb, mown, mrecv, ar, wg, wrow, wcol, part, rec_e, rec_x,
    ld_sem, w_sem, v_sem, r_sem, ms_sem, mr_sem, as_sem, arr_sem, ws_sem, wr_sem, rs_sem, chunk_sem, across_sem, ag_sem, near_sem, far_sem,
):
    z = lax.axis_index("row")
    c = lax.axis_index("col")
    blk = mint.shape[2]
    nc, width = part.shape[1], part.shape[3]
    hi = z // 2
    is_mid = lax.rem(z + hi, 2)

    def row_of(mirrored):
        return mirrored + hi * (3 - 2 * mirrored)

    def to_row(src, dst, send, recv, row):
        return pltpu.make_async_remote_copy(
            src_ref=src, dst_ref=dst, send_sem=send, recv_sem=recv, device_id={"row": row}, device_id_type=MESH)

    def sent(buf, sem, n):
        src = buf if n is None else buf.at[:n]
        to_row(src, src, sem, sem, z).wait_send()

    cross, end = 3 - z, 3 * hi
    order = (2 - hi, 3 - 3 * hi, is_mid * end + (1 - is_mid) * (1 + hi), z)

    def load(hbm, buf, s, sem):
        return pltpu.make_async_copy(hbm.at[:, pl.ds(pl.multiple_of(s * blk, blk), blk)], buf.at[s], sem)

    barrier = pltpu.get_barrier_semaphore()
    load(m_hbm, mint, order[0], ld_sem.at[0]).start()

    def tell(sem, row):
        pl.semaphore_signal(sem, inc=1, device_id={"row": row}, device_id_type=MESH)

    @pl.when(is_mid == 1)
    def _():
        tell(barrier, cross)
        tell(barrier, end)

    @pl.when(is_mid == 0)
    def _():
        tell(barrier, 1 + hi)

    for off in range(1, 4):
        pl.semaphore_signal(barrier, inc=1, device_id={"col": lax.rem(c + off, 4)}, device_id_type=MESH)
    def observed(s, k, scores):
        cols = pl.ds(pl.multiple_of(k * width, width), width)
        return jnp.where(mint[s, :, cols] > 0, rbuf[s, :, cols] - scores, 0.0).astype(BF)

    def send_mask(s):
        to_row(mown.at[s], mrecv.at[z], ms_sem, mr_sem.at[z], s).start()

    first = jnp.zeros(w0_ref.shape[::-1], F32)
    for j, s in enumerate(order):
        load(m_hbm, mint, s, ld_sem.at[j]).wait()
        for k in range(nc):
            m = mint[s, :, k * width:(k + 1) * width].astype(F32).astype(BF)
            mown[s, k] = m
            if j == 3:
                mrecv[z, k] = m
        if j == 0:
            pl.semaphore_wait(barrier, 4 + is_mid)

            @pl.when(is_mid == 1)
            def _():
                tell(far_sem, cross)
                tell(near_sem, end)

            @pl.when(is_mid == 0)
            def _():
                pl.semaphore_wait(near_sem, 1)

        if j == 1:
            pl.semaphore_wait(far_sem, 1)

            @pl.when(is_mid == 1)
            def _():
                tell(far_sem, end)

        if j < 3:
            send_mask(s)
        if j == 0:
            pltpu.make_async_copy(w0_hbm, w0_ref, w_sem).start()
            for i, other in enumerate(order):
                if i:
                    load(m_hbm, mint, other, ld_sem.at[i]).start()
                load(v0_hbm, v0b, other, v_sem).start()
                load(r_hbm, rbuf, other, r_sem).start()
            pltpu.make_async_copy(w0_hbm, w0_ref, w_sem).wait()
            w0 = w0_ref[...]
            rows0 = w0.T.astype(BF)
            pltpu.make_async_copy(v0b, v0b, v_sem).wait()
            pltpu.make_async_copy(rbuf, rbuf, r_sem).wait()
        for k in range(nc):
            cols = slice(k * width, (k + 1) * width)
            f = v0b[s, :, cols].astype(BF)
            fb[s, :, cols] = f
            first = first + mm(observed(s, k, mm(rows0, f, 1, 0)), f, 1, 1)

    def user_product(x):
        rows = x.T.astype(BF)
        acc = jnp.zeros((x.shape[1], x.shape[0]), F32)
        for s in range(4):
            for k in range(0, nc, 2):
                f = fb[s, :, k * width:(k + 2) * width]
                mask = jnp.concatenate([mown[s, k], mown[s, k + 1]], axis=1)
                acc = acc + mm(mask * mm(rows, f, 1, 0).astype(BF), f, 1, 1)
        return acc.T

    def to_col(rnd, off):
        peer = lax.rem(c + off, 4)
        return pltpu.make_async_remote_copy(
            src_ref=ar.at[rnd, c], dst_ref=ar.at[rnd, c], send_sem=as_sem, recv_sem=arr_sem.at[lax.rem(rnd, 2), c],
            device_id={"col": peer}, device_id_type=MESH)

    def from_col(rnd, off):
        peer = lax.rem(c + off, 4)
        return pltpu.make_async_remote_copy(
            src_ref=ar.at[rnd, peer], dst_ref=ar.at[rnd, peer], send_sem=as_sem,
            recv_sem=arr_sem.at[lax.rem(rnd, 2), peer], device_id={"col": peer}, device_id_type=MESH)

    def sum_cols(rnd, x):
        ar[rnd, c] = x
        for off in range(1, 4):
            to_col(rnd, off).start()
        for off in range(1, 4):
            from_col(rnd, off).wait_recv()
        return (ar[rnd, 0] + ar[rnd, 1]) + (ar[rnd, 2] + ar[rnd, 3])

    res = sum_cols(0, first.T) - ridge_u * w0

    def user_step(i, state):
        x, r, p, res_sq = state

        q = sum_cols(i + 1, user_product(p)) + ridge_u * p
        step_size = res_sq / col_sum(p, q)
        x = x + step_size * p
        r = r - step_size * q
        new_sq = col_sum(r, r)
        p = r + (new_sq / res_sq) * p
        return x, r, p, new_sq

    w1 = lax.fori_loop(0, CG_STEPS, user_step, (w0, res, res, col_sum(res, res)))[0]
    u_out[...] = w1

    def give(src_row, row):
        return to_row(wg.at[src_row], wg.at[src_row], ws_sem, wr_sem.at[src_row], row)

    wg[z] = w1.astype(BF)

    @pl.when(is_mid == 0)
    def _():
        give(z, 1 + hi).start()

    @pl.when(is_mid == 1)
    def _():
        give(z, cross).start()
        give(z, end).start()

    own_rows = w1.T.astype(BF)
    own_cols = w1.astype(BF)

    def rs_out(s, k):
        return to_row(part.at[s, k], rec_e.at[s, k], rs_sem, chunk_sem.at[s, k], 1 + hi)

    def rs_cross(s, k, sem):
        return to_row(part.at[s, k], rec_x.at[s, k], rs_sem, sem, cross)

    def rs_end(s, k):
        return to_row(part.at[s, k], rec_x.at[s, k], rs_sem, chunk_sem.at[s, k], end)

    def each(body, n=nc):
        def step(k, carry):
            body(k)
            return carry

        lax.fori_loop(0, n, step, 0)

    def outer_first(j):
        return row_of(3 - j)

    def partial_sums(k):
        for j in range(4):
            s = outer_first(j)
            f = fb[s, :, pl.ds(pl.multiple_of(k * width, width), width)]
            part[s, k] = mm(own_cols, observed(s, k, mm(own_rows, f, 1, 0)), 1, 0)

        @pl.when(is_mid == 0)
        def _():
            for j in range(3):
                rs_out(outer_first(j), k).start()

    each(partial_sums)

    def gather():
        for off in range(1, 4):
            peer = lax.rem(z + off, 4)
            @pl.when((is_mid == 0) | (peer != end))
            def _():
                give(peer, end).wait_recv()

            @pl.when((is_mid == 1) & (peer != end))
            def _():
                give(peer, end).start()

            to_row(mown.at[peer], mrecv.at[peer], ms_sem, mr_sem.at[peer], peer).wait_recv()
        users = own_rows.shape[0]
        for s in range(4):
            wrow[s * users:(s + 1) * users] = wg[s].astype(F32).T.astype(BF)
            wcol[:, s * users:(s + 1) * users] = wg[s]

    def cols_of(s, k):
        return pl.ds(pl.multiple_of(s * blk + k * width, width), width)

    def solve_items(k, residual):
        start = v0b[z, :, pl.ds(pl.multiple_of(k * width, width), width)]

        def apply_a(p):
            pb = p.astype(BF)
            users = wrow.shape[0] // 2
            halves = []
            for i in range(2):
                mask = jnp.concatenate([mrecv[2 * i, k], mrecv[2 * i + 1, k]], axis=0)
                halves.append(mask * mm(wrow[i * users:(i + 1) * users], pb, 1, 0).astype(BF))
            return mm(wcol[...], jnp.concatenate(halves, axis=0), 1, 0) + ridge_i * p

        vout[:, cols_of(z, k)] = cg_steps(apply_a, start, residual - ridge_i * start)

    def ag(s, k, row):
        chunk = vout.at[:, cols_of(s, k)]
        return to_row(chunk, chunk, ag_sem, chunk_sem.at[s, k], row)

    s0, s1, s2, s3 = (row_of(m) for m in range(4))

    @pl.when(is_mid == 0)
    def _():
        inner = 1 + hi

        def own(k):
            rs_end(s0, k).wait_recv()
            solve_items(k, part[s0, k] + rec_x[s0, k])
            ag(s0, k, inner).start()

        def take(s):
            def body(k):
                ag(s, k, inner).wait_recv()

            return body

        gather()
        each(own)
        for s in (s1, s2, s3):
            each(take(s))
        sent(wg, ws_sem, 1)
        sent(part, rs_sem, 3)
        sent(vout.at[:, :blk], ag_sem, None)

    @pl.when(is_mid == 1)
    def _():
        def outer_to_cross(s, sem):
            def body(k):
                rs_out(s, k).wait_recv()
                part[s, k] = part[s, k] + rec_e[s, k]
                rs_cross(s, k, sem(k)).start()

            return body

        def cross_to_end(k):
            rs_cross(s0, k, chunk_sem.at[s0, k]).wait_recv()
            part[s0, k] = part[s0, k] + rec_x[s0, k]
            rs_end(s0, k).start()

        def own(k):
            rs_out(s1, k).wait_recv()
            rs_cross(s1, k, across_sem.at[k]).wait_recv()
            solve_items(k, part[s1, k] + (rec_e[s1, k] + rec_x[s1, k]))
            ag(s1, k, cross).start()
            ag(s1, k, end).start()

        def relay(s, row):
            def body(k):
                ag(s, k, row).wait_recv()
                ag(s, k, row).start()

            return body

        def held_relay(s, row):
            def body(k):
                ag(s, k, row).wait_recv()

                @pl.when(lax.rem(c, 2) == 0)
                def _():
                    ag(s, k, row).start()

                @pl.when(lax.rem(c, 2) == 1)
                def _():
                    if k >= HOLD:
                        ag(s, k - HOLD, row).start()
                    if k == nc - 1:
                        for i in range(nc - HOLD, nc):
                            ag(s, i, row).start()

            return body

        relays = (
            outer_to_cross(s3, lambda k: chunk_sem.at[s3, k]), outer_to_cross(s2, lambda k: across_sem.at[k]), cross_to_end, relay(s2, end), held_relay(s0, cross), relay(s3, end),
        )
        give(end, cross).wait_recv()
        give(end, cross).start()
        for kind, k in RELAYS[0]:
            relays[kind](k)
        gather()

        def step(j):
            own(j)
            for i in range(nc):
                @pl.when(j == i)
                def _():
                    for kind, k in RELAYS[i + 1]:
                        relays[kind](k)

        each(step)
        sent(wg, ws_sem, 4)
        sent(wg, ws_sem, 1)
        sent(part, rs_sem, 3)
        for _ in range(5):
            sent(vout.at[:, :blk], ag_sem, None)

    sent(mown, ms_sem, 3)
    sent(ar.at[:, :3], as_sem, None)


def finish_kernel(u_in, v_in, u_out, v_out, sem):
    copies = [pltpu.make_async_copy(v_in, v_out, sem.at[0]), pltpu.make_async_copy(u_in, u_out, sem.at[1])]
    for copy in copies:
        copy.start()
    for copy in copies:
        copy.wait()


def solution(mesh):
    row_size = mesh.shape["row"]
    col_size = mesh.shape["col"]
    assert row_size == 4 and col_size == 4
    grid_spec = P(("part", "row"), "col")
    user_spec = P(("part", "row"), None)
    item_spec = P(("part", "col"), None)

    def local_step(ratings, mask, user_blk, item_blk):
        users, items = ratings.shape
        rank = user_blk.shape[1]
        blk = items // row_size
        width = blk // CHUNKS
        ridge_u, ridge_i = RIDGE_WEIGHT * (items * col_size), RIDGE_WEIGHT * (users * row_size)
        vmem, any_space = pl.BlockSpec(memory_space=pltpu.VMEM), pl.BlockSpec(memory_space=pl.ANY)
        dma = pltpu.SemaphoreType.DMA
        sums = pltpu.VMEM((4, CHUNKS, rank, width), F32)
        user_new, item_new = pl.pallas_call(
            functools.partial(kernel, ridge_u, ridge_i),
            out_shape=(pltpu.VMEM((rank, users), F32), pltpu.VMEM((rank, items), F32)),
            in_specs=[any_space, any_space, any_space, any_space],
            out_specs=(vmem, vmem),
            scratch_shapes=[
                pltpu.VMEM((rank, users), F32),
                pltpu.VMEM((4, users, blk), jnp.int32),
                pltpu.VMEM((4, users, blk), F32),
                pltpu.VMEM((4, rank, blk), F32),
                pltpu.VMEM((4, rank, blk), BF),
                pltpu.VMEM((4, CHUNKS, users, width), BF),
                pltpu.VMEM((4, CHUNKS, users, width), BF),
                pltpu.VMEM((CG_STEPS + 1, 4, rank, users), F32),
                pltpu.VMEM((4, rank, users), BF),
                pltpu.VMEM((4 * users, rank), BF),
                pltpu.VMEM((rank, 4 * users), BF),
                sums, sums, sums,
                dma((4,)), dma, dma, dma, dma, dma((4,)), dma, dma((2, 4)), dma, dma((4,)),
                dma, dma((4, CHUNKS)), dma((CHUNKS,)), dma,
                pltpu.SemaphoreType.REGULAR, pltpu.SemaphoreType.REGULAR,
            ],
            compiler_params=pltpu.CompilerParams(
                collective_id=0, has_side_effects=True, vmem_limit_bytes=56 * 2**20),
            name="als_sweep",
        )(ratings, mask, user_blk.T, item_blk.T)
        user_new, item_new = pl.pallas_call(
            finish_kernel,
            out_shape=(jax.ShapeDtypeStruct((rank, users), F32), jax.ShapeDtypeStruct((rank, items), F32)),
            in_specs=[vmem, vmem],
            out_specs=(any_space, any_space),
            scratch_shapes=[dma((2,))],
            name="write_out",
        )(*(pltpu.with_memory_space_constraint(x, pltpu.VMEM) for x in (user_new, item_new)))
        return user_new.T, item_new.T

    return jax.shard_map(local_step, mesh=mesh, in_specs=(grid_spec, grid_spec, user_spec, item_spec), out_specs=(user_spec, item_spec), check_vma=False)
```

```python
import functools

import jax
import jax.numpy as jnp
from jax import lax
from jax.experimental import pallas as pl
from jax.experimental.pallas import tpu as pltpu
from jax.sharding import PartitionSpec as P

CG_STEPS = 4
RIDGE_WEIGHT = 0.0005
CHUNKS = 8
FAR_SUM, NEAR_SUM, END_SUM, NEAR_RES, END_RES, FAR_RES = range(6)
RELAYS = (
    ((FAR_SUM, 0), (NEAR_SUM, 0), (FAR_SUM, 1), (NEAR_SUM, 1), (FAR_SUM, 2), (END_SUM, 0), (NEAR_SUM, 2)),
    ((END_SUM, 1), (FAR_SUM, 3)),
    ((NEAR_SUM, 3), (END_SUM, 2)),
    ((FAR_SUM, 4), (NEAR_RES, 0), (NEAR_SUM, 4), (END_SUM, 3), (NEAR_RES, 1), (FAR_SUM, 5)),
    ((NEAR_SUM, 5), (NEAR_RES, 2), (END_SUM, 4), (FAR_SUM, 6)),
    ((NEAR_SUM, 6), (END_SUM, 5), (NEAR_RES, 3), (FAR_SUM, 7)),
    ((NEAR_SUM, 7), (END_SUM, 6), (NEAR_RES, 4), (END_RES, 0)),
    ((END_SUM, 7), (END_RES, 1), (END_RES, 2), (NEAR_RES, 5), (END_RES, 3)),
    ((END_RES, 4), (FAR_RES, 0), (END_RES, 5), (NEAR_RES, 6), (END_RES, 6), (FAR_RES, 1), (FAR_RES, 2), (FAR_RES, 3), (END_RES, 7), (NEAR_RES, 7), (FAR_RES, 4), (FAR_RES, 5), (FAR_RES, 6), (FAR_RES, 7)),
)
HOLD = 3
BF, F32 = jnp.bfloat16, jnp.float32
MESH = pl.DeviceIdType.MESH


def mm(a, b, contract_a, contract_b):
    return lax.dot_general(a, b, (((contract_a,), (contract_b,)), ((), ())), preferred_element_type=F32)


def col_sum(a, b):
    return jnp.sum(a * b, axis=0, keepdims=True)


def cg_steps(apply_a, start, residual):
    direction = residual
    estimate = start
    res_sq = col_sum(residual, residual)
    for cg_step in range(CG_STEPS):
        gram_dir = apply_a(direction)
        step_size = res_sq / col_sum(direction, gram_dir)
        estimate = estimate + step_size * direction
        if cg_step + 1 < CG_STEPS:
            residual = residual - step_size * gram_dir
            new_sq = col_sum(residual, residual)
            direction = residual + (new_sq / res_sq) * direction
            res_sq = new_sq
    return estimate


def kernel(
    ridge_u, ridge_i,
    r_hbm, m_hbm, w0_hbm, v0_hbm,
    u_out, vout,
    w0_ref, mint, rbuf, v0b, fb, mown, mrecv, ar, wg, wrow, wcol, part, rec_e, rec_x,
    ld_sem, w_sem, v_sem, r_sem, ms_sem, mr_sem, as_sem, arr_sem, ws_sem, wr_sem, rs_sem, chunk_sem, across_sem, ag_sem, near_sem, far_sem,
):
    z = lax.axis_index("row")
    c = lax.axis_index("col")
    blk = mint.shape[2]
    nc, width = part.shape[1], part.shape[3]
    hi = z // 2
    is_mid = lax.rem(z + hi, 2)

    def row_of(mirrored):
        return mirrored + hi * (3 - 2 * mirrored)

    def to_row(src, dst, send, recv, row):
        return pltpu.make_async_remote_copy(
            src_ref=src, dst_ref=dst, send_sem=send, recv_sem=recv, device_id={"row": row}, device_id_type=MESH)

    def sent(buf, sem, n):
        src = buf if n is None else buf.at[:n]
        to_row(src, src, sem, sem, z).wait_send()

    cross, end = 3 - z, 3 * hi
    order = (2 - hi, 3 - 3 * hi, is_mid * end + (1 - is_mid) * (1 + hi), z)

    def load(hbm, buf, s, sem):
        return pltpu.make_async_copy(hbm.at[:, pl.ds(pl.multiple_of(s * blk, blk), blk)], buf.at[s], sem)

    barrier = pltpu.get_barrier_semaphore()
    load(m_hbm, mint, order[0], ld_sem.at[0]).start()

    def tell(sem, row):
        pl.semaphore_signal(sem, inc=1, device_id={"row": row}, device_id_type=MESH)

    @pl.when(is_mid == 1)
    def _():
        tell(barrier, cross)
        tell(barrier, end)

    @pl.when(is_mid == 0)
    def _():
        tell(barrier, 1 + hi)

    for off in range(1, 4):
        pl.semaphore_signal(barrier, inc=1, device_id={"col": lax.rem(c + off, 4)}, device_id_type=MESH)
    def observed(s, k, scores):
        cols = pl.ds(pl.multiple_of(k * width, width), width)
        return jnp.where(mint[s, :, cols] > 0, rbuf[s, :, cols] - scores, 0.0).astype(BF)

    def send_mask(s):
        to_row(mown.at[s], mrecv.at[z], ms_sem, mr_sem, s).start()

    first = jnp.zeros(w0_ref.shape[::-1], F32)
    for j, s in enumerate(order):
        load(m_hbm, mint, s, ld_sem.at[j]).wait()
        for k in range(nc):
            m = mint[s, :, k * width:(k + 1) * width].astype(F32).astype(BF)
            mown[s, k] = m
            if j == 3:
                mrecv[z, k] = m
        if j == 0:
            pl.semaphore_wait(barrier, 4 + is_mid)

            @pl.when(is_mid == 1)
            def _():
                tell(far_sem, cross)
                tell(near_sem, end)

            @pl.when(is_mid == 0)
            def _():
                pl.semaphore_wait(near_sem, 1)

        if j == 1:
            pl.semaphore_wait(far_sem, 1)

            @pl.when(is_mid == 1)
            def _():
                tell(far_sem, end)

        if j < 3:
            send_mask(s)
        if j == 0:
            pltpu.make_async_copy(w0_hbm, w0_ref, w_sem).start()
            for i, other in enumerate(order):
                if i:
                    load(m_hbm, mint, other, ld_sem.at[i]).start()
                load(v0_hbm, v0b, other, v_sem).start()
                load(r_hbm, rbuf, other, r_sem).start()
            pltpu.make_async_copy(w0_hbm, w0_ref, w_sem).wait()
            w0 = w0_ref[...]
            rows0 = w0.T.astype(BF)
            pltpu.make_async_copy(v0b, v0b, v_sem).wait()
            pltpu.make_async_copy(rbuf, rbuf, r_sem).wait()
        for k in range(nc):
            cols = slice(k * width, (k + 1) * width)
            f = v0b[s, :, cols].astype(BF)
            fb[s, :, cols] = f
            first = first + mm(observed(s, k, mm(rows0, f, 1, 0)), f, 1, 1)

    def user_product(x):
        rows = x.T.astype(BF)
        acc = jnp.zeros((x.shape[1], x.shape[0]), F32)
        for s in range(4):
            for k in range(0, nc, 2):
                f = fb[s, :, k * width:(k + 2) * width]
                mask = jnp.concatenate([mown[s, k], mown[s, k + 1]], axis=1)
                acc = acc + mm(mask * mm(rows, f, 1, 0).astype(BF), f, 1, 1)
        return acc.T

    def to_col(rnd, off):
        peer = lax.rem(c + off, 4)
        return pltpu.make_async_remote_copy(
            src_ref=ar.at[rnd, c], dst_ref=ar.at[rnd, c], send_sem=as_sem, recv_sem=arr_sem.at[lax.rem(rnd, 2)],
            device_id={"col": peer}, device_id_type=MESH)

    def sum_cols(rnd, x):
        ar[rnd, c] = x
        for off in range(1, 4):
            to_col(rnd, off).start()
        others = ar.at[rnd, :3]
        to_row(others, others, as_sem, arr_sem.at[lax.rem(rnd, 2)], z).wait_recv()
        return (ar[rnd, 0] + ar[rnd, 1]) + (ar[rnd, 2] + ar[rnd, 3])

    res = sum_cols(0, first.T) - ridge_u * w0

    def user_step(i, state):
        x, r, p, res_sq = state

        q = sum_cols(i + 1, user_product(p)) + ridge_u * p
        step_size = res_sq / col_sum(p, q)
        x = x + step_size * p
        r = r - step_size * q
        new_sq = col_sum(r, r)
        p = r + (new_sq / res_sq) * p
        return x, r, p, new_sq

    w1 = lax.fori_loop(0, CG_STEPS, user_step, (w0, res, res, col_sum(res, res)))[0]
    u_out[...] = w1

    def give(src_row, row):
        return to_row(wg.at[src_row], wg.at[src_row], ws_sem, wr_sem.at[src_row], row)

    wg[z] = w1.astype(BF)

    @pl.when(is_mid == 0)
    def _():
        give(z, 1 + hi).start()

    @pl.when(is_mid == 1)
    def _():
        give(z, cross).start()
        give(z, end).start()

    own_rows = w1.T.astype(BF)
    own_cols = w1.astype(BF)

    def rs_out(s, k):
        return to_row(part.at[s, k], rec_e.at[s, k], rs_sem, chunk_sem.at[s, k], 1 + hi)

    def rs_cross(s, k, sem):
        return to_row(part.at[s, k], rec_x.at[s, k], rs_sem, sem, cross)

    def rs_end(s, k):
        return to_row(part.at[s, k], rec_x.at[s, k], rs_sem, chunk_sem.at[s, k], end)

    def each(body, n=nc):
        def step(k, carry):
            body(k)
            return carry

        lax.fori_loop(0, n, step, 0)

    def outer_first(j):
        return row_of(3 - j)

    def partial_sums(k):
        for j in range(4):
            s = outer_first(j)
            f = fb[s, :, pl.ds(pl.multiple_of(k * width, width), width)]
            part[s, k] = mm(own_cols, observed(s, k, mm(own_rows, f, 1, 0)), 1, 0)

        @pl.when(is_mid == 0)
        def _():
            for j in range(3):
                rs_out(outer_first(j), k).start()

    each(partial_sums)

    def gather():
        for off in range(1, 4):
            peer = lax.rem(z + off, 4)
            @pl.when((is_mid == 0) | (peer != end))
            def _():
                give(peer, end).wait_recv()

            @pl.when((is_mid == 1) & (peer != end))
            def _():
                give(peer, end).start()

        masks = mrecv.at[:3]
        to_row(masks, masks, ms_sem, mr_sem, z).wait_recv()
        users = own_rows.shape[0]
        for s in range(4):
            wrow[s * users:(s + 1) * users] = wg[s].astype(F32).T.astype(BF)
            wcol[:, s * users:(s + 1) * users] = wg[s]

    def cols_of(s, k):
        return pl.ds(pl.multiple_of(s * blk + k * width, width), width)

    def solve_items(k, residual):
        start = v0b[z, :, pl.ds(pl.multiple_of(k * width, width), width)]

        def apply_a(p):
            pb = p.astype(BF)
            users = wrow.shape[0] // 2
            halves = []
            for i in range(2):
                mask = jnp.concatenate([mrecv[2 * i, k], mrecv[2 * i + 1, k]], axis=0)
                halves.append(mask * mm(wrow[i * users:(i + 1) * users], pb, 1, 0).astype(BF))
            return mm(wcol[...], jnp.concatenate(halves, axis=0), 1, 0) + ridge_i * p

        vout[:, cols_of(z, k)] = cg_steps(apply_a, start, residual - ridge_i * start)

    def ag(s, k, row):
        chunk = vout.at[:, cols_of(s, k)]
        return to_row(chunk, chunk, ag_sem, chunk_sem.at[s, k], row)

    s0, s1, s2, s3 = (row_of(m) for m in range(4))

    def sent_early():
        sent(part, rs_sem, 3)
        sent(mown, ms_sem, 3)
        sent(ar.at[:, :3], as_sem, None)

    @pl.when(is_mid == 0)
    def _():
        inner = 1 + hi

        def own(k):
            rs_end(s0, k).wait_recv()
            solve_items(k, part[s0, k] + rec_x[s0, k])
            ag(s0, k, inner).start()

        def take(s):
            def body(k):
                ag(s, k, inner).wait_recv()

            return body

        gather()
        each(own)
        for s in (s1, s2):
            each(take(s))
        sent_early()
        each(take(s3))
        sent(wg, ws_sem, 1)
        sent(vout.at[:, :blk], ag_sem, None)

    @pl.when(is_mid == 1)
    def _():
        def outer_to_cross(s, sem):
            def body(k):
                rs_out(s, k).wait_recv()
                part[s, k] = part[s, k] + rec_e[s, k]
                rs_cross(s, k, sem(k)).start()

            return body

        def cross_to_end(k):
            rs_cross(s0, k, chunk_sem.at[s0, k]).wait_recv()
            part[s0, k] = part[s0, k] + rec_x[s0, k]
            rs_end(s0, k).start()

        def own(k):
            rs_out(s1, k).wait_recv()
            rs_cross(s1, k, across_sem.at[k]).wait_recv()
            solve_items(k, part[s1, k] + (rec_e[s1, k] + rec_x[s1, k]))
            ag(s1, k, cross).start()
            ag(s1, k, end).start()

        def relay(s, row):
            def body(k):
                ag(s, k, row).wait_recv()
                ag(s, k, row).start()

            return body

        def held_relay(s, row):
            def body(k):
                ag(s, k, row).wait_recv()

                @pl.when(lax.rem(c, 2) == 0)
                def _():
                    ag(s, k, row).start()

                @pl.when(lax.rem(c, 2) == 1)
                def _():
                    if k >= HOLD:
                        ag(s, k - HOLD, row).start()
                    if k == nc - 1:
                        for i in range(nc - HOLD, nc):
                            ag(s, i, row).start()

            return body

        relays = (
            outer_to_cross(s3, lambda k: chunk_sem.at[s3, k]), outer_to_cross(s2, lambda k: across_sem.at[k]), cross_to_end, relay(s2, end), held_relay(s0, cross), relay(s3, end),
        )
        give(end, cross).wait_recv()
        give(end, cross).start()
        for kind, k in RELAYS[0]:
            relays[kind](k)
        gather()

        def step(j):
            own(j)
            for i in range(nc):
                @pl.when(j == i)
                def _():
                    for kind, k in RELAYS[i + 1]:
                        relays[kind](k)

        each(step)
        sent(wg, ws_sem, 4)
        sent(wg, ws_sem, 1)
        sent_early()
        for _ in range(5):
            sent(vout.at[:, :blk], ag_sem, None)


def finish_kernel(u_in, v_in, u_out, v_out, sem):
    copies = [pltpu.make_async_copy(v_in, v_out, sem.at[0]), pltpu.make_async_copy(u_in, u_out, sem.at[1])]
    for copy in copies:
        copy.start()
    for copy in copies:
        copy.wait()


def solution(mesh):
    row_size = mesh.shape["row"]
    col_size = mesh.shape["col"]
    assert row_size == 4 and col_size == 4
    grid_spec = P(("part", "row"), "col")
    user_spec = P(("part", "row"), None)
    item_spec = P(("part", "col"), None)

    def local_step(ratings, mask, user_blk, item_blk):
        users, items = ratings.shape
        rank = user_blk.shape[1]
        blk = items // row_size
        width = blk // CHUNKS
        ridge_u, ridge_i = RIDGE_WEIGHT * (items * col_size), RIDGE_WEIGHT * (users * row_size)
        vmem, any_space = pl.BlockSpec(memory_space=pltpu.VMEM), pl.BlockSpec(memory_space=pl.ANY)
        dma = pltpu.SemaphoreType.DMA
        sums = pltpu.VMEM((4, CHUNKS, rank, width), F32)
        user_new, item_new = pl.pallas_call(
            functools.partial(kernel, ridge_u, ridge_i),
            out_shape=(pltpu.VMEM((rank, users), F32), pltpu.VMEM((rank, items), F32)),
            in_specs=[any_space, any_space, any_space, any_space],
            out_specs=(vmem, vmem),
            scratch_shapes=[
                pltpu.VMEM((rank, users), F32),
                pltpu.VMEM((4, users, blk), jnp.int32),
                pltpu.VMEM((4, users, blk), F32),
                pltpu.VMEM((4, rank, blk), F32),
                pltpu.VMEM((4, rank, blk), BF),
                pltpu.VMEM((4, CHUNKS, users, width), BF),
                pltpu.VMEM((4, CHUNKS, users, width), BF),
                pltpu.VMEM((CG_STEPS + 1, 4, rank, users), F32),
                pltpu.VMEM((4, rank, users), BF),
                pltpu.VMEM((4 * users, rank), BF),
                pltpu.VMEM((rank, 4 * users), BF),
                sums, sums, sums,
                dma((4,)), dma, dma, dma, dma, dma, dma, dma((2,)), dma, dma((4,)),
                dma, dma((4, CHUNKS)), dma((CHUNKS,)), dma,
                pltpu.SemaphoreType.REGULAR, pltpu.SemaphoreType.REGULAR,
            ],
            compiler_params=pltpu.CompilerParams(
                collective_id=0, has_side_effects=True, vmem_limit_bytes=56 * 2**20),
            name="als_sweep",
        )(ratings, mask, user_blk.T, item_blk.T)
        user_new, item_new = pl.pallas_call(
            finish_kernel,
            out_shape=(jax.ShapeDtypeStruct((rank, users), F32), jax.ShapeDtypeStruct((rank, items), F32)),
            in_specs=[vmem, vmem],
            out_specs=(any_space, any_space),
            scratch_shapes=[dma((2,))],
            name="write_out",
        )(*(pltpu.with_memory_space_constraint(x, pltpu.VMEM) for x in (user_new, item_new)))
        return user_new.T, item_new.T

    return jax.shard_map(local_step, mesh=mesh, in_specs=(grid_spec, grid_spec, user_spec, item_spec), out_specs=(user_spec, item_spec), check_vma=False)
```

```python
import functools

import jax
import jax.numpy as jnp
from jax import lax
from jax.experimental import pallas as pl
from jax.experimental.pallas import tpu as pltpu
from jax.sharding import PartitionSpec as P

CG_STEPS = 4
RIDGE_WEIGHT = 0.0005
CHUNKS = 8
FAR_SUM, NEAR_SUM, END_SUM, NEAR_RES, END_RES, FAR_RES = range(6)
RELAYS = (
    ((FAR_SUM, 0), (NEAR_SUM, 0), (FAR_SUM, 1), (NEAR_SUM, 1), (FAR_SUM, 2), (END_SUM, 0), (NEAR_SUM, 2)),
    ((END_SUM, 1), (FAR_SUM, 3)),
    ((NEAR_SUM, 3), (END_SUM, 2)),
    ((FAR_SUM, 4), (NEAR_RES, 0), (NEAR_SUM, 4), (END_SUM, 3), (NEAR_RES, 1), (FAR_SUM, 5)),
    ((NEAR_SUM, 5), (NEAR_RES, 2), (END_SUM, 4), (FAR_SUM, 6)),
    ((NEAR_SUM, 6), (END_SUM, 5), (NEAR_RES, 3), (FAR_SUM, 7)),
    ((NEAR_SUM, 7), (END_SUM, 6), (NEAR_RES, 4), (END_RES, 0)),
    ((END_SUM, 7), (END_RES, 1), (END_RES, 2), (NEAR_RES, 5), (END_RES, 3)),
    ((END_RES, 4), (FAR_RES, 0), (END_RES, 5), (NEAR_RES, 6), (END_RES, 6), (FAR_RES, 1), (FAR_RES, 2), (FAR_RES, 3), (END_RES, 7), (NEAR_RES, 7), (FAR_RES, 4), (FAR_RES, 5), (FAR_RES, 6), (FAR_RES, 7)),
)
HOLD = 3
BF, F32 = jnp.bfloat16, jnp.float32
MESH = pl.DeviceIdType.MESH


def mm(a, b, contract_a, contract_b):
    return lax.dot_general(a, b, (((contract_a,), (contract_b,)), ((), ())), preferred_element_type=F32)


def col_sum(a, b):
    return jnp.sum(a * b, axis=0, keepdims=True)


def cg_steps(apply_a, start, residual):
    direction = residual
    estimate = start
    res_sq = col_sum(residual, residual)
    for cg_step in range(CG_STEPS):
        gram_dir = apply_a(direction)
        step_size = res_sq / col_sum(direction, gram_dir)
        estimate = estimate + step_size * direction
        if cg_step + 1 < CG_STEPS:
            residual = residual - step_size * gram_dir
            new_sq = col_sum(residual, residual)
            direction = residual + (new_sq / res_sq) * direction
            res_sq = new_sq
    return estimate


def kernel(
    ridge_u, ridge_i,
    r_hbm, m_hbm, w0_hbm, v0_hbm,
    u_out, vout,
    w0_ref, mint, rbuf, v0b, fb, mown, mrecv, ar, wg, wrow, wcol, part, rec_e, rec_x,
    ld_sem, w_sem, v_sem, r_sem, ms_sem, mr_sem, as_sem, arr_sem, ws_sem, wr_sem, rs_sem, chunk_sem, across_sem, ag_sem, near_sem, far_sem,
):
    z = lax.axis_index("row")
    c = lax.axis_index("col")
    blk = mint.shape[2]
    nc, width = part.shape[1], part.shape[3]
    hi = z // 2
    is_mid = lax.rem(z + hi, 2)

    def row_of(mirrored):
        return mirrored + hi * (3 - 2 * mirrored)

    def to_row(src, dst, send, recv, row):
        return pltpu.make_async_remote_copy(
            src_ref=src, dst_ref=dst, send_sem=send, recv_sem=recv, device_id={"row": row}, device_id_type=MESH)

    def sent(buf, sem, n):
        src = buf if n is None else buf.at[:n]
        to_row(src, src, sem, sem, z).wait_send()

    cross, end = 3 - z, 3 * hi
    order = (2 - hi, 3 - 3 * hi, is_mid * end + (1 - is_mid) * (1 + hi), z)

    def load(hbm, buf, s, sem):
        return pltpu.make_async_copy(hbm.at[:, pl.ds(pl.multiple_of(s * blk, blk), blk)], buf.at[s], sem)

    barrier = pltpu.get_barrier_semaphore()
    load(m_hbm, mint, order[0], ld_sem.at[0]).start()

    def tell(sem, row):
        pl.semaphore_signal(sem, inc=1, device_id={"row": row}, device_id_type=MESH)

    @pl.when(is_mid == 1)
    def _():
        tell(barrier, cross)
        tell(barrier, end)

    @pl.when(is_mid == 0)
    def _():
        tell(barrier, 1 + hi)

    for off in range(1, 4):
        pl.semaphore_signal(barrier, inc=1, device_id={"col": lax.rem(c + off, 4)}, device_id_type=MESH)
    def observed(s, k, scores):
        cols = pl.ds(pl.multiple_of(k * width, width), width)
        return jnp.where(mint[s, :, cols] > 0, rbuf[s, :, cols] - scores, 0.0).astype(BF)

    def send_mask(s):
        to_row(mown.at[s], mrecv.at[z], ms_sem, mr_sem, s).start()

    first = jnp.zeros(w0_ref.shape[::-1], F32)
    for j, s in enumerate(order):
        if j == 0:
            load(m_hbm, mint, s, ld_sem.at[0]).wait()
        elif j == 1:
            pltpu.make_async_copy(mint.at[:3], mint.at[:3], ld_sem.at[1]).wait()
        for k in range(nc):
            m = mint[s, :, k * width:(k + 1) * width].astype(F32).astype(BF)
            mown[s, k] = m
            if j == 3:
                mrecv[z, k] = m
        if j == 0:
            pl.semaphore_wait(barrier, 4 + is_mid)

            @pl.when(is_mid == 1)
            def _():
                tell(far_sem, cross)
                tell(near_sem, end)

            @pl.when(is_mid == 0)
            def _():
                pl.semaphore_wait(near_sem, 1)

        if j == 1:
            pl.semaphore_wait(far_sem, 1)

            @pl.when(is_mid == 1)
            def _():
                tell(far_sem, end)

        if j < 3:
            send_mask(s)
        if j == 0:
            pltpu.make_async_copy(w0_hbm, w0_ref, w_sem).start()
            for i, other in enumerate(order):
                if i:
                    load(m_hbm, mint, other, ld_sem.at[1]).start()
                load(v0_hbm, v0b, other, v_sem).start()
                load(r_hbm, rbuf, other, r_sem).start()
            pltpu.make_async_copy(w0_hbm, w0_ref, w_sem).wait()
            w0 = w0_ref[...]
            rows0 = w0.T.astype(BF)
            pltpu.make_async_copy(v0b, v0b, v_sem).wait()
            pltpu.make_async_copy(rbuf, rbuf, r_sem).wait()
        for k in range(nc):
            cols = slice(k * width, (k + 1) * width)
            f = v0b[s, :, cols].astype(BF)
            fb[s, :, cols] = f
            first = first + mm(observed(s, k, mm(rows0, f, 1, 0)), f, 1, 1)

    def user_product(x):
        rows = x.T.astype(BF)
        acc = jnp.zeros((x.shape[1], x.shape[0]), F32)
        for s in range(4):
            for k in range(0, nc, 2):
                f = fb[s, :, k * width:(k + 2) * width]
                mask = jnp.concatenate([mown[s, k], mown[s, k + 1]], axis=1)
                acc = acc + mm(mask * mm(rows, f, 1, 0).astype(BF), f, 1, 1)
        return acc.T

    def to_col(rnd, off):
        peer = lax.rem(c + off, 4)
        return pltpu.make_async_remote_copy(
            src_ref=ar.at[rnd, c], dst_ref=ar.at[rnd, c], send_sem=as_sem, recv_sem=arr_sem.at[lax.rem(rnd, 2)],
            device_id={"col": peer}, device_id_type=MESH)

    def sum_cols(rnd, x):
        ar[rnd, c] = x
        for off in range(1, 4):
            to_col(rnd, off).start()
        others = ar.at[rnd, :3]
        to_row(others, others, as_sem, arr_sem.at[lax.rem(rnd, 2)], z).wait_recv()
        return (ar[rnd, 0] + ar[rnd, 1]) + (ar[rnd, 2] + ar[rnd, 3])

    res = sum_cols(0, first.T) - ridge_u * w0

    def user_step(i, state):
        x, r, p, res_sq = state

        q = sum_cols(i + 1, user_product(p)) + ridge_u * p
        step_size = res_sq / col_sum(p, q)
        x = x + step_size * p
        r = r - step_size * q
        new_sq = col_sum(r, r)
        p = r + (new_sq / res_sq) * p
        return x, r, p, new_sq

    w1 = lax.fori_loop(0, CG_STEPS, user_step, (w0, res, res, col_sum(res, res)))[0]
    u_out[...] = w1

    def give(src_row, row):
        return to_row(wg.at[src_row], wg.at[src_row], ws_sem, wr_sem.at[src_row], row)

    wg[z] = w1.astype(BF)

    @pl.when(is_mid == 0)
    def _():
        give(z, 1 + hi).start()

    @pl.when(is_mid == 1)
    def _():
        give(z, cross).start()
        give(z, end).start()

    own_rows = w1.T.astype(BF)
    own_cols = w1.astype(BF)

    def rs_out(s, k):
        return to_row(part.at[s, k], rec_e.at[s, k], rs_sem, chunk_sem.at[s, k], 1 + hi)

    def rs_cross(s, k, sem):
        return to_row(part.at[s, k], rec_x.at[s, k], rs_sem, sem, cross)

    def rs_end(s, k):
        return to_row(part.at[s, k], rec_x.at[s, k], rs_sem, chunk_sem.at[s, k], end)

    def each(body, n=nc):
        def step(k, carry):
            body(k)
            return carry

        lax.fori_loop(0, n, step, 0)

    def outer_first(j):
        return row_of(3 - j)

    def partial_sums(k):
        for j in range(4):
            s = outer_first(j)
            f = fb[s, :, pl.ds(pl.multiple_of(k * width, width), width)]
            part[s, k] = mm(own_cols, observed(s, k, mm(own_rows, f, 1, 0)), 1, 0)

        @pl.when(is_mid == 0)
        def _():
            for j in range(3):
                rs_out(outer_first(j), k).start()

    each(partial_sums)

    def gather():
        for off in range(1, 4):
            peer = lax.rem(z + off, 4)
            @pl.when((is_mid == 0) | (peer != end))
            def _():
                give(peer, end).wait_recv()

            @pl.when((is_mid == 1) & (peer != end))
            def _():
                give(peer, end).start()

        masks = mrecv.at[:3]
        to_row(masks, masks, ms_sem, mr_sem, z).wait_recv()
        users = own_rows.shape[0]
        for s in range(4):
            wrow[s * users:(s + 1) * users] = wg[s].astype(F32).T.astype(BF)
            wcol[:, s * users:(s + 1) * users] = wg[s]

    def cols_of(s, k):
        return pl.ds(pl.multiple_of(s * blk + k * width, width), width)

    def solve_items(k, residual):
        start = v0b[z, :, pl.ds(pl.multiple_of(k * width, width), width)]

        def apply_a(p):
            pb = p.astype(BF)
            users = wrow.shape[0] // 2
            halves = []
            for i in range(2):
                mask = jnp.concatenate([mrecv[2 * i, k], mrecv[2 * i + 1, k]], axis=0)
                halves.append(mask * mm(wrow[i * users:(i + 1) * users], pb, 1, 0).astype(BF))
            return mm(wcol[...], jnp.concatenate(halves, axis=0), 1, 0) + ridge_i * p

        vout[:, cols_of(z, k)] = cg_steps(apply_a, start, residual - ridge_i * start)

    def ag(s, k, row):
        chunk = vout.at[:, cols_of(s, k)]
        return to_row(chunk, chunk, ag_sem, chunk_sem.at[s, k], row)

    s0, s1, s2, s3 = (row_of(m) for m in range(4))

    def sent_early():
        sent(part, rs_sem, 3)
        sent(mown, ms_sem, 3)
        sent(ar.at[:, :3], as_sem, None)

    @pl.when(is_mid == 0)
    def _():
        inner = 1 + hi

        def own(k):
            rs_end(s0, k).wait_recv()
            solve_items(k, part[s0, k] + rec_x[s0, k])
            ag(s0, k, inner).start()

        def take(s):
            def body(k):
                ag(s, k, inner).wait_recv()

            return body

        gather()
        each(own)
        for s in (s1, s2):
            each(take(s))
        sent_early()
        each(take(s3))
        sent(wg, ws_sem, 1)
        sent(vout.at[:, :blk], ag_sem, None)

    @pl.when(is_mid == 1)
    def _():
        def outer_to_cross(s, sem):
            def body(k):
                rs_out(s, k).wait_recv()
                part[s, k] = part[s, k] + rec_e[s, k]
                rs_cross(s, k, sem(k)).start()

            return body

        def cross_to_end(k):
            rs_cross(s0, k, chunk_sem.at[s0, k]).wait_recv()
            part[s0, k] = part[s0, k] + rec_x[s0, k]
            rs_end(s0, k).start()

        def own(k):
            rs_out(s1, k).wait_recv()
            rs_cross(s1, k, across_sem.at[k]).wait_recv()
            solve_items(k, part[s1, k] + (rec_e[s1, k] + rec_x[s1, k]))
            ag(s1, k, cross).start()
            ag(s1, k, end).start()

        def relay(s, row):
            def body(k):
                ag(s, k, row).wait_recv()
                ag(s, k, row).start()

            return body

        def held_relay(s, row):
            def body(k):
                ag(s, k, row).wait_recv()

                @pl.when(lax.rem(c, 2) == 0)
                def _():
                    ag(s, k, row).start()

                @pl.when(lax.rem(c, 2) == 1)
                def _():
                    if k >= HOLD:
                        ag(s, k - HOLD, row).start()
                    if k == nc - 1:
                        for i in range(nc - HOLD, nc):
                            ag(s, i, row).start()

            return body

        relays = (
            outer_to_cross(s3, lambda k: chunk_sem.at[s3, k]), outer_to_cross(s2, lambda k: across_sem.at[k]), cross_to_end, relay(s2, end), held_relay(s0, cross), relay(s3, end),
        )
        give(end, cross).wait_recv()
        give(end, cross).start()
        for kind, k in RELAYS[0]:
            relays[kind](k)
        gather()

        def step(j):
            own(j)
            for i in range(nc):
                @pl.when(j == i)
                def _():
                    for kind, k in RELAYS[i + 1]:
                        relays[kind](k)

        each(step)
        sent(wg, ws_sem, 4)
        sent(wg, ws_sem, 1)
        sent_early()
        for _ in range(5):
            sent(vout.at[:, :blk], ag_sem, None)


def finish_kernel(u_in, v_in, u_out, v_out, sem):
    copies = [pltpu.make_async_copy(v_in, v_out, sem.at[0]), pltpu.make_async_copy(u_in, u_out, sem.at[1])]
    for copy in copies:
        copy.start()
    for copy in copies:
        copy.wait()


def solution(mesh):
    row_size = mesh.shape["row"]
    col_size = mesh.shape["col"]
    assert row_size == 4 and col_size == 4
    grid_spec = P(("part", "row"), "col")
    user_spec = P(("part", "row"), None)
    item_spec = P(("part", "col"), None)

    def local_step(ratings, mask, user_blk, item_blk):
        users, items = ratings.shape
        rank = user_blk.shape[1]
        blk = items // row_size
        width = blk // CHUNKS
        ridge_u, ridge_i = RIDGE_WEIGHT * (items * col_size), RIDGE_WEIGHT * (users * row_size)
        vmem, any_space = pl.BlockSpec(memory_space=pltpu.VMEM), pl.BlockSpec(memory_space=pl.ANY)
        dma = pltpu.SemaphoreType.DMA
        sums = pltpu.VMEM((4, CHUNKS, rank, width), F32)
        user_new, item_new = pl.pallas_call(
            functools.partial(kernel, ridge_u, ridge_i),
            out_shape=(pltpu.VMEM((rank, users), F32), pltpu.VMEM((rank, items), F32)),
            in_specs=[any_space, any_space, any_space, any_space],
            out_specs=(vmem, vmem),
            scratch_shapes=[
                pltpu.VMEM((rank, users), F32),
                pltpu.VMEM((4, users, blk), jnp.int32),
                pltpu.VMEM((4, users, blk), F32),
                pltpu.VMEM((4, rank, blk), F32),
                pltpu.VMEM((4, rank, blk), BF),
                pltpu.VMEM((4, CHUNKS, users, width), BF),
                pltpu.VMEM((4, CHUNKS, users, width), BF),
                pltpu.VMEM((CG_STEPS + 1, 4, rank, users), F32),
                pltpu.VMEM((4, rank, users), BF),
                pltpu.VMEM((4 * users, rank), BF),
                pltpu.VMEM((rank, 4 * users), BF),
                sums, sums, sums,
                dma((2,)), dma, dma, dma, dma, dma, dma, dma((2,)), dma, dma((4,)),
                dma, dma((4, CHUNKS)), dma((CHUNKS,)), dma,
                pltpu.SemaphoreType.REGULAR, pltpu.SemaphoreType.REGULAR,
            ],
            compiler_params=pltpu.CompilerParams(
                collective_id=0, has_side_effects=True, vmem_limit_bytes=56 * 2**20),
            name="als_sweep",
        )(ratings, mask, user_blk.T, item_blk.T)
        user_new, item_new = pl.pallas_call(
            finish_kernel,
            out_shape=(jax.ShapeDtypeStruct((rank, users), F32), jax.ShapeDtypeStruct((rank, items), F32)),
            in_specs=[vmem, vmem],
            out_specs=(any_space, any_space),
            scratch_shapes=[dma((2,))],
            name="write_out",
        )(*(pltpu.with_memory_space_constraint(x, pltpu.VMEM) for x in (user_new, item_new)))
        return user_new.T, item_new.T

    return jax.shard_map(local_step, mesh=mesh, in_specs=(grid_spec, grid_spec, user_spec, item_spec), out_specs=(user_spec, item_spec), check_vma=False)
```
